8 devices in a mesh: data: 1 (over z), expert: 8 (over y, x, core).
Axes of the slice: x: 2, y: 2, z: 1, core: 2. Of those that a mesh axis runs over, the one named last changes fastest.
Arguments:
- x_in: bfloat16 [32768, 384], P(('data', 'expert'))
- expert_idx: int32 [32768, 1], P(('data', 'expert'))
- gate_weight: float32 [32768, 1], P(('data', 'expert'))
- grad_y: bfloat16 [32768, 384], P(('data', 'expert'))
- w_in: bfloat16 [128, 384, 1536], P('expert')
- w_out: bfloat16 [128, 1536, 384], P('expert')
Outputs:
- output 1: bfloat16 [32768, 384], P(('data', 'expert'))
- output 2: bfloat16 [32768, 384], P(('data', 'expert'))
- output 3: float32 [32768, 1], P(('data', 'expert'))
- output 4: bfloat16 [128, 384, 1536], P(('data', 'expert'))
- output 5: bfloat16 [128, 1536, 384], P(('data', 'expert'))
All inputs are finite; a program needn't handle non-finite values.
Results may differ from the reference program's by a relative error of at most 0.0107263.
Values are sent between devices in bfloat16 or wider.
A program may use at most 1 GiB of HBM per device.

```python
import jax
import jax.numpy as jnp
from jax import lax

TOKENS = 4096
GROUP_SIZE = 8
D_MODEL = 384
D_FF = 1536
EXPERTS = 128
TOP_K = 1
CAPACITY = 320

LOCAL_EXPERTS = EXPERTS // GROUP_SIZE
DEVICE_PAIRS = TOKENS * TOP_K
FAIR_SHARE = DEVICE_PAIRS // GROUP_SIZE
GROUP_ROWS = GROUP_SIZE * TOKENS
GROUP_PAIRS = GROUP_ROWS * TOP_K


def route_device(rng_key, hot_offset):
    key_perm, key_shift, key_quartet, key_pick, key_shuffle = jax.random.split(rng_key, 5)
    owner_perm = jax.random.permutation(key_perm, GROUP_SIZE)
    shift_size = jax.random.randint(key_shift, (GROUP_SIZE // 2,), 0, FAIR_SHARE + 1)
    shift_size = shift_size.at[0].set(FAIR_SHARE)
    per_owner = jnp.full((GROUP_SIZE,), FAIR_SHARE, jnp.int32)
    per_owner = per_owner.at[owner_perm[0::2]].add(shift_size).at[owner_perm[1::2]].add(-shift_size)
    owner_dev = jnp.searchsorted(jnp.cumsum(per_owner), jnp.arange(DEVICE_PAIRS, dtype=jnp.int32), side='right')
    quartet = jax.random.randint(key_quartet, (DEVICE_PAIRS,), 0, LOCAL_EXPERTS // 4)
    pick_draw = jax.random.randint(key_pick, (DEVICE_PAIRS,), 0, 8)
    hot_slot = hot_offset[owner_dev, quartet]
    within = jnp.where(pick_draw < 5, hot_slot, (hot_slot + pick_draw - 4) % 4)
    expert_id = owner_dev * LOCAL_EXPERTS + quartet * 4 + within
    return expert_id[jax.random.permutation(key_shuffle, DEVICE_PAIRS)].astype(jnp.int32)


def setup_inputs(seed: int = 0, part: int = 0) -> dict:
    part_key = jax.random.fold_in(jax.random.key(seed), part)
    key_x, key_gate, key_dy, key_hot, key_route = jax.random.split(part_key, 5)
    key_in, key_out = jax.random.split(jax.random.key(seed + 1), 2)
    hot_offset = jax.random.randint(key_hot, (GROUP_SIZE, LOCAL_EXPERTS // 4), 0, 4)
    route_keys = jax.random.split(key_route, GROUP_SIZE)
    expert_idx = jax.vmap(route_device, in_axes=(0, None))(route_keys, hot_offset).reshape(GROUP_ROWS, TOP_K)
    x_in = jax.random.normal(key_x, (GROUP_ROWS, D_MODEL), jnp.float32).astype(jnp.bfloat16)
    gate_weight = jax.random.uniform(key_gate, (GROUP_ROWS, TOP_K), jnp.float32, 0.5, 1.5) * TOP_K ** -0.5
    grad_y = jax.random.normal(key_dy, (GROUP_ROWS, D_MODEL), jnp.float32).astype(jnp.bfloat16)
    w_in = (jax.random.normal(key_in, (EXPERTS, D_MODEL, D_FF), jnp.float32) * D_MODEL ** -0.5).astype(jnp.bfloat16)
    w_out = (jax.random.normal(key_out, (EXPERTS, D_FF, D_MODEL), jnp.float32) * D_FF ** -0.5).astype(jnp.bfloat16)
    return {'x_in': x_in, 'expert_idx': expert_idx, 'gate_weight': gate_weight, 'grad_y': grad_y, 'w_in': w_in, 'w_out': w_out}


def reference(x_in, expert_idx, gate_weight, grad_y, w_in, w_out):
    flat_idx = expert_idx.reshape(GROUP_PAIRS)
    pair_ids = jnp.arange(GROUP_PAIRS, dtype=jnp.int32)
    sort_order = jnp.argsort(flat_idx, stable=True)
    counts = jnp.zeros((EXPERTS,), jnp.int32).at[flat_idx].add(1)
    starts = jnp.cumsum(counts) - counts
    sorted_rank = pair_ids - starts[flat_idx[sort_order]]
    pair_slot = jnp.zeros((GROUP_PAIRS,), jnp.int32).at[sort_order].set(sorted_rank)
    dest_row = jnp.where(pair_slot < CAPACITY, flat_idx * CAPACITY + pair_slot, EXPERTS * CAPACITY)
    source_pair = jnp.full((EXPERTS * CAPACITY,), GROUP_PAIRS, jnp.int32).at[dest_row].set(pair_ids, mode='drop')
    exp_rows = jnp.take(x_in, source_pair // TOP_K, axis=0, mode='fill', fill_value=0).reshape(EXPERTS, CAPACITY, D_MODEL)
    scaled_grad = (gate_weight[:, :, None] * grad_y[:, None, :].astype(jnp.float32)).astype(jnp.bfloat16).reshape(GROUP_PAIRS, D_MODEL)
    grad_rows = jnp.take(scaled_grad, source_pair, axis=0, mode='fill', fill_value=0).reshape(EXPERTS, CAPACITY, D_MODEL)

    def expert_pass(operands):
        rows_in, rows_grad, weight_in, weight_out = operands
        pre_act = jnp.dot(rows_in, weight_in, preferred_element_type=jnp.float32)
        act_full, gelu_pull = jax.vjp(jax.nn.gelu, pre_act)
        act_bf = act_full.astype(jnp.bfloat16)
        rows_out = jnp.dot(act_bf, weight_out, preferred_element_type=jnp.float32).astype(jnp.bfloat16)
        grad_act = jnp.dot(rows_grad, weight_out.T, preferred_element_type=jnp.float32).astype(jnp.bfloat16)
        grad_pre = gelu_pull(grad_act.astype(jnp.float32))[0].astype(jnp.bfloat16)
        grad_weight_out = jnp.dot(act_bf.T, rows_grad, preferred_element_type=jnp.float32).astype(jnp.bfloat16)
        grad_weight_in = jnp.dot(rows_in.T, grad_pre, preferred_element_type=jnp.float32).astype(jnp.bfloat16)
        grad_in = jnp.dot(grad_pre, weight_in.T, preferred_element_type=jnp.float32).astype(jnp.bfloat16)
        return rows_out, grad_in, grad_weight_in, grad_weight_out

    out_rows, grad_in_rows, grad_w_in, grad_w_out = lax.map(expert_pass, (exp_rows, grad_rows, w_in, w_out))
    out_pair = jnp.take(out_rows.reshape(EXPERTS * CAPACITY, D_MODEL), dest_row, axis=0, mode='fill', fill_value=0).reshape(GROUP_ROWS, TOP_K, D_MODEL).astype(jnp.float32)
    grad_pair = jnp.take(grad_in_rows.reshape(EXPERTS * CAPACITY, D_MODEL), dest_row, axis=0, mode='fill', fill_value=0).reshape(GROUP_ROWS, TOP_K, D_MODEL).astype(jnp.float32)
    y_out = (x_in.astype(jnp.float32) + jnp.sum(gate_weight[:, :, None] * out_pair, axis=1)).astype(jnp.bfloat16)
    grad_gate = jnp.sum(grad_y.astype(jnp.float32)[:, None, :] * out_pair, axis=2)
    grad_x = (grad_y.astype(jnp.float32) + jnp.sum(grad_pair, axis=1)).astype(jnp.bfloat16)
    return y_out, grad_x, grad_gate, grad_w_in, grad_w_out
```

```python
import functools

import jax
import jax.numpy as jnp
from jax import lax
from jax.experimental import pallas as pl
from jax.experimental.pallas import tpu as pltpu
from jax.sharding import PartitionSpec as P

CAP_NUM = 5
CAP_DEN = 4
PAIR_FACTOR = 2
CHUNKS = 2
HALVES = (768,)
CORES = 2
LANES = 128
BIG = 60 * 2 ** 20
F32 = jnp.float32
BF16 = jnp.bfloat16
I32 = jnp.int32
GELU_C = 0.7978845608028654
GELU_A = 0.044715
VMEM = pl.BlockSpec(memory_space=pltpu.VMEM)
SMEM = pl.BlockSpec(memory_space=pltpu.SMEM)
ANY = pl.BlockSpec(memory_space=pl.ANY)


def local_ranks(flat_idx, num_experts):
    one_hot = (flat_idx[:, None] == jnp.arange(num_experts, dtype=jnp.int32)[None, :]).astype(jnp.int32)
    running = jnp.cumsum(one_hot, axis=0)
    return jnp.sum((running - one_hot) * one_hot, axis=1), running[-1]


def exchange_maps(flat_idx, local_rank, counts_all, my_index, local_experts, capacity, pair_cap):
    groups, num_experts = counts_all.shape
    n_pairs = flat_idx.shape[0]
    through = jnp.cumsum(counts_all, axis=0)
    before = through - counts_all
    kept_all = jnp.clip(capacity - before, 0, counts_all)
    before_mine = lax.dynamic_index_in_dim(before, my_index, 0, keepdims=False)
    kept_grid = lax.dynamic_index_in_dim(kept_all, my_index, 0, keepdims=False).reshape(groups, local_experts)
    send_start = (jnp.cumsum(kept_grid, axis=1) - kept_grid).reshape(num_experts)
    pair_slot = before_mine[flat_idx] + local_rank
    target = jnp.where(pair_slot < capacity, (flat_idx // local_experts) * pair_cap + send_start[flat_idx] + local_rank, groups * pair_cap)
    send_src = jnp.full((groups * pair_cap,), n_pairs, jnp.int32).at[target].set(jnp.arange(n_pairs, dtype=jnp.int32), mode='drop')
    first_expert = my_index * local_experts
    through_own = lax.dynamic_slice_in_dim(through, first_expert, local_experts, axis=1)
    before_own = lax.dynamic_slice_in_dim(before, first_expert, local_experts, axis=1)
    kept_own = lax.dynamic_slice_in_dim(kept_all, first_expert, local_experts, axis=1)
    start_own = jnp.cumsum(kept_own, axis=1) - kept_own
    slot_ids = jnp.arange(capacity, dtype=jnp.int32)
    source_dev = jnp.sum((through_own.T[:, None, :] <= slot_ids[None, :, None]).astype(jnp.int32), axis=2)
    filled = slot_ids[None, :] < jnp.minimum(through_own[-1], capacity)[:, None]
    source_dev = jnp.minimum(source_dev, groups - 1)
    start_at = jnp.take_along_axis(start_own.T, source_dev, axis=1)
    before_at = jnp.take_along_axis(before_own.T, source_dev, axis=1)
    recv_pos = jnp.where(filled, source_dev * pair_cap + start_at + slot_ids[None, :] - before_at, groups * pair_cap).reshape(local_experts * capacity)
    back_src = jnp.full((groups * pair_cap,), local_experts * capacity, jnp.int32).at[recv_pos].set(jnp.arange(local_experts * capacity, dtype=jnp.int32), mode='drop')
    return target, send_src, recv_pos, back_src


def exchange(rows):
    return lax.all_to_all(rows, 'expert', 0, 0, tiled=True)


def gather_rows(table, positions):
    return jnp.take(table, positions, axis=0, mode='fill', fill_value=0)


def padded_pass(groups, x_in, expert_idx, gate_weight, grad_y, w_in, w_out):
    n_tokens, top_k = expert_idx.shape
    local_experts, d_model = w_in.shape[0], w_in.shape[1]
    num_experts = local_experts * groups
    n_pairs = n_tokens * top_k
    capacity = (CAP_NUM * n_pairs * groups) // (CAP_DEN * num_experts)
    pair_cap = PAIR_FACTOR * n_pairs // groups
    my_index = lax.axis_index('expert')
    flat_idx = expert_idx.reshape(n_pairs)
    local_rank, counts = local_ranks(flat_idx, num_experts)
    counts_all = lax.all_gather(counts, 'expert')
    target, send_src, recv_pos, back_src = exchange_maps(flat_idx, local_rank, counts_all, my_index, local_experts, capacity, pair_cap)
    exp_rows = gather_rows(exchange(gather_rows(x_in, send_src // top_k)), recv_pos).reshape(local_experts, capacity, d_model)
    pre_act = jnp.einsum('lcd,ldf->lcf', exp_rows, w_in, preferred_element_type=jnp.float32)
    act_full, gelu_pull = jax.vjp(jax.nn.gelu, pre_act)
    act_bf = act_full.astype(jnp.bfloat16)
    out_rows = jnp.einsum('lcf,lfd->lcd', act_bf, w_out, preferred_element_type=jnp.float32).astype(jnp.bfloat16)
    back_out = gather_rows(out_rows.reshape(local_experts * capacity, d_model), back_src)
    out_pair = gather_rows(exchange(back_out), target).reshape(n_tokens, top_k, d_model)
    y_out = (x_in.astype(jnp.float32) + jnp.sum(gate_weight[:, :, None] * out_pair, axis=1)).astype(jnp.bfloat16)
    grad_gate = jnp.einsum('tkd,td->tk', out_pair, grad_y, preferred_element_type=jnp.float32)
    scaled_grad = (gate_weight[:, :, None] * grad_y[:, None, :]).astype(jnp.bfloat16).reshape(n_pairs, d_model)
    grad_rows = gather_rows(exchange(gather_rows(scaled_grad, send_src)), recv_pos).reshape(local_experts, capacity, d_model)
    grad_act = jnp.einsum('lcd,lfd->lcf', grad_rows, w_out, preferred_element_type=jnp.float32).astype(jnp.bfloat16)
    grad_pre = gelu_pull(grad_act.astype(jnp.float32))[0].astype(jnp.bfloat16)
    grad_w_out = jnp.einsum('lcf,lcd->lfd', act_bf, grad_rows, preferred_element_type=jnp.float32).astype(jnp.bfloat16)
    grad_w_in = jnp.einsum('lcd,lcf->ldf', exp_rows, grad_pre, preferred_element_type=jnp.float32).astype(jnp.bfloat16)
    grad_in_rows = jnp.einsum('lcf,ldf->lcd', grad_pre, w_in, preferred_element_type=jnp.float32).astype(jnp.bfloat16)
    back_grad = gather_rows(grad_in_rows.reshape(local_experts * capacity, d_model), back_src)
    grad_pair = gather_rows(exchange(back_grad), target).reshape(n_tokens, top_k, d_model)
    grad_x = (grad_y.astype(jnp.float32) + jnp.sum(grad_pair, axis=1, dtype=jnp.float32)).astype(jnp.bfloat16)
    return y_out, grad_x, grad_gate, grad_w_in, grad_w_out


def iota(shape, dim):
    return lax.broadcasted_iota(jnp.int32, shape, dim)


def exact_dot(a, b):
    return jnp.dot(a, b, preferred_element_type=F32, precision=lax.Precision.HIGHEST)


def xor_chip(a, b):
    return lax.rem(lax.div(a, 2) + lax.div(b, 2), 2) * 2 + lax.rem(lax.rem(a, 2) + lax.rem(b, 2), 2)


def sum_rows(m):
    return jnp.sum(m, axis=0, keepdims=True)


def count_kernel(groups, idx_ref, rank_ref, every_ref, mine, every, send_sem, recv_sem):
    me = lax.axis_index('expert')
    core = lax.rem(me, CORES)
    rows = idx_ref.shape[0] // CORES
    barrier = pltpu.get_barrier_semaphore()
    for s in range(1, groups):
        pl.semaphore_signal(barrier, inc=1, device_id={'expert': lax.rem(me + s, groups)}, device_id_type=pl.DeviceIdType.MESH)

    def one_hot(r):
        return jnp.where(iota((LANES, LANES), 0) == idx_ref[pl.ds(r, 1), :], 1.0, 0.0)

    seen = jnp.zeros((LANES, LANES), F32)
    for r in range(rows):
        seen = seen + one_hot(core * rows + r)
    counts = lax.dot_general(jnp.ones((8, LANES), BF16), seen.astype(BF16), (((1,), (1,)), ((), ())), preferred_element_type=F32)
    mine[...] = counts.astype(I32)
    every[pl.ds(me, 1)] = counts.astype(I32)[None]
    pl.semaphore_wait(barrier, groups - 1)
    copies = []
    for s in range(1, groups):
        copy = pltpu.make_async_remote_copy(src_ref=mine, dst_ref=every.at[me], send_sem=send_sem.at[s], recv_sem=recv_sem.at[s],
                                            device_id={'expert': lax.rem(me + s, groups)}, device_id_type=pl.DeviceIdType.MESH)
        copy.start()
        copies.append(copy)
    earlier = jnp.where(iota((LANES, LANES), 0) < iota((LANES, LANES), 1), 1.0, 0.0)
    mix = jnp.concatenate([earlier, jnp.ones((LANES, LANES), F32)], axis=0).astype(BF16)
    done = jnp.zeros((LANES, LANES), F32)
    for r in range(rows * CORES):
        hot = one_hot(r)
        rank = jnp.dot(jnp.concatenate([hot, done], axis=1).astype(BF16), mix, preferred_element_type=F32)
        rank_ref[r:r + 1, :] = sum_rows(hot * rank).astype(I32)
        done = done + hot
    for copy in copies:
        copy.wait()
    every_ref[...] = every[:, 0, :]


def chip_tables(cnt, capacity, local_experts):
    groups = cnt.shape[0]
    part = local_experts // CHUNKS
    source = iota((groups, LANES), 0)
    before = jnp.zeros((groups, LANES), F32)
    for i in range(groups - 1):
        before = before + jnp.where(source > i, cnt[i:i + 1, :], 0.0)
    kept = jnp.clip(capacity - before, 0.0, cnt)
    chips = groups // CORES
    k2 = jnp.concatenate([kept[CORES * c:CORES * c + 1] + kept[CORES * c + 1:CORES * c + 2] for c in range(chips)], axis=0)
    b0 = jnp.concatenate([before[CORES * c:CORES * c + 1] for c in range(chips)], axis=0)
    e0, e1 = iota((LANES, LANES), 0), iota((LANES, LANES), 1)
    chip_experts = CORES * local_experts
    same = (lax.div(e0, chip_experts) == lax.div(e1, chip_experts)) & (lax.rem(lax.div(e0, part), CHUNKS) == lax.rem(lax.div(e1, part), CHUNKS))
    start = exact_dot(jnp.concatenate([k2, k2], axis=0), jnp.where(same & (e0 < e1), 1.0, 0.0))[:chips]
    return k2, b0, start


def need_kernel(capacity, local_experts, every_ref, need_ref):
    k2, _, start = chip_tables(every_ref[...].astype(F32), capacity, local_experts)
    away = iota(k2.shape, 0) != lax.div(iota(k2.shape, 1), CORES * local_experts)
    longest = jnp.max(jnp.where(away, start + k2, 0.0), axis=0, keepdims=True)
    need_ref[...] = jnp.broadcast_to(jnp.max(longest, axis=1, keepdims=True), (1, LANES)).astype(I32)


def map_kernel(capacity, local_experts, half, idx_ref, rank_ref, every_ref, inv_ref, recv_ref, ret_ref, fpos_ref, fill_ref, cols, fall):
    me = lax.axis_index('expert')
    core, chip = lax.rem(me, CORES), lax.div(me, CORES)
    rows = idx_ref.shape[0] // CORES
    n_tokens = rows * LANES
    part = local_experts // CHUNKS
    k2, b0, start = chip_tables(every_ref[...].astype(F32), capacity, local_experts)
    chips = k2.shape[0]
    mine = iota(k2.shape, 0) == chip
    pad = jnp.zeros((LANES - 3 * chips, LANES), F32)
    cols[...] = jnp.transpose(jnp.concatenate([k2, b0, start, pad], axis=0)).astype(I32)
    look = jnp.concatenate([sum_rows(jnp.where(mine, v, 0.0)) for v in (k2, b0, start)], axis=0)
    high = jnp.floor(look * (1.0 / LANES))
    look = jnp.concatenate([high, look - LANES * high, jnp.zeros((2, LANES), F32)], axis=0).astype(BF16)
    part_rows = part * capacity
    slot_rows = (capacity + LANES - 1) // LANES
    region = (chips - 1) * half + slot_rows * part * LANES
    final = 2 * (chips - 1) * half + CORES * part_rows
    n_high = (CHUNKS * region // LANES + 7) // 8 * 8
    acc = jnp.zeros((2 * n_high, LANES), F32)
    lane = iota((1, LANES), 1)
    nt = (((1,), (1,)), ((), ()))
    for r in range(rows * CORES):
        e = idx_ref[r:r + 1, :]
        hot = jnp.where(iota((LANES, LANES), 0) == e, 1.0, 0.0).astype(BF16)
        found = jnp.dot(look, hot, preferred_element_type=F32).astype(I32)
        found = found[0:3] * LANES + found[3:6]
        rank = rank_ref[r:r + 1, :]
        slot = found[1:2] + rank
        q = found[2:3] + rank
        owner = lax.div(e, local_experts)
        group = lax.rem(lax.div(e, part), CHUNKS)
        el = lax.rem(e, part)
        m = xor_chip(lax.div(owner, CORES), chip)
        here = q - core * half
        slot_at = (chips - 1) * half + lax.div(slot, LANES) * (part * LANES) + el * LANES + lax.rem(slot, LANES)
        pos = group * region + jnp.where(m > 0, (m - 1) * half + here, slot_at)
        kept = rank < found[0:1]
        in_half = (here >= 0) & (here < half)
        valid = kept & (((m > 0) & in_half) | ((m == 0) & (owner == me)))
        pos = jnp.where(valid, pos, -1)
        hi = jnp.where(iota((n_high, LANES), 0) == jnp.where(valid, lax.div(pos, LANES), -1), 1.0, 0.0)
        lo = jnp.where(iota((LANES, LANES), 0) == lax.rem(pos, LANES), 1.0, 0.0).astype(BF16)
        row_id = (r % rows + jnp.where(core == r // rows, 0, rows)).astype(F32)
        left = jnp.concatenate([hi * row_id, hi * lane.astype(F32)], axis=0).astype(BF16)
        acc = acc + lax.dot_general(left, lo, nt, preferred_element_type=F32)
        other = (chips - 1) * half
        in_list = jnp.where(in_half, 0, other) + (m - 1) * half + lax.rem(q, half)
        in_own = 2 * other + jnp.where(owner == me, 0, part_rows) + el * capacity + slot
        fall[r:r + 1, :] = jnp.where(kept, group * final + jnp.where(m > 0, in_list, in_own), CHUNKS * final)
    fpos_ref[...] = fall[pl.ds(core * rows, rows), :]
    inv = (acc[:n_high] * LANES + acc[n_high:]).astype(I32)
    inv_ref[...] = inv
    lists = (chips - 1) * half
    for c in range(CHUNKS):
        col = cols[pl.ds(me * local_experts + c * part, part), :]
        total = col[:, 0:1]
        for i in range(1, chips):
            total = total + col[:, i:i + 1]
        fill_ref[c * part:(c + 1) * part, :] = jnp.broadcast_to(total, (part, LANES))
        for j in range(slot_rows):
            s = j * LANES + iota((part, LANES), 1)
            first = (c * region + lists) // LANES + j * part
            at = jnp.zeros((part, LANES), I32)
            for src in range(chips):
                rel = s - col[:, chips + src:chips + src + 1]
                q = col[:, 2 * chips + src:2 * chips + src + 1] + rel
                here = q - core * half
                away = xor_chip(src, chip)
                remote = jnp.where((here >= 0) & (here < half), 0, lists) + (away - 1) * half + lax.rem(jnp.maximum(q, 0), half)
                own = 2 * lists + inv[first:first + part]
                at = jnp.where((rel >= 0) & (rel < col[:, src:src + 1]), jnp.where(away > 0, remote, own), at)
            row = (c * slot_rows + j) * part
            recv_ref[row:row + part, :] = at
        q = core * half + iota((part, half), 1)
        for m in range(1, chips):
            src = xor_chip(m, chip)
            at = jnp.zeros((1, half), I32)
            for o in range(CORES):
                col = cols[pl.ds((chip * CORES + o) * local_experts + c * part, part), :]

                def pick(base):
                    return jnp.sum(jnp.where(iota((part, LANES), 1) == base + src, col, 0), axis=1, keepdims=True)

                rel = q - pick(2 * chips)
                base = jnp.where(core == o, 0, part_rows) + iota((part, 1), 0) * capacity
                hit = (rel >= 0) & (rel < pick(0))
                at = at + sum_rows(jnp.where(hit, base + rel + pick(chips), 0))
            ret_ref[c * (chips - 1) + m - 1:c * (chips - 1) + m, :] = at


def column(row):
    return jnp.transpose(jnp.broadcast_to(row, (LANES, LANES)))


def build_kernel(tile, x_ref, gate_ref, dy_ref, out_ref):
    step = pl.program_id(0)
    for q in range(tile // LANES):
        block = pl.ds(q * LANES, LANES)
        gate = column(gate_ref[pl.ds(step * (tile // LANES) + q, 1), :])
        gate = jnp.concatenate([gate] * (x_ref.shape[1] // LANES), axis=1)
        out_ref[block, 0, :] = x_ref[block, :]
        out_ref[block, 1, :] = (gate * dy_ref[block, :].astype(F32)).astype(BF16)


def copy_rows(n, unroll, index, table, rows, first=0):
    def body(b, carry):
        for u in range(unroll):
            rows[pl.ds(first + b * unroll + u, 1)] = table[pl.ds(index(b * unroll + u), 1)]
        return carry

    lax.fori_loop(0, n // unroll, body, 0)


def load_tables(pieces, table, sems):
    at = 0
    copies = []
    for i, piece in enumerate(pieces):
        copy = pltpu.make_async_copy(piece, table.at[pl.ds(at, piece.shape[0])], sems.at[i])
        copy.start()
        copies.append(copy)
        at += piece.shape[0]
    for copy in copies:
        copy.wait()


def pick_kernel(n_tables, first, pos_ref, *refs):
    pieces, outs, (table, sems) = refs[:n_tables], refs[n_tables:-2], refs[-2:]
    load_tables(pieces, table, sems)
    at = first
    for out in outs:
        copy_rows(out.shape[0], 16, lambda t, at=at: pos_ref[at + t], table, out)
        at += out.shape[0]


def expert_kernel(n_tables, n_extra, first, part, capacity, f_tile, fill_ref, pos_ref, w_in_ref, w_out_ref, *refs):
    pieces = refs[:n_tables]
    out_ref, gw_in_ref, gw_out_ref, table, rows, sems = refs[n_tables + n_extra:]
    j = pl.program_id(0)

    @pl.when(j == 0)
    def _():
        load_tables(pieces, table, sems)

    for s in range(0, capacity, LANES):
        n = min(LANES, capacity - s)
        base = ((first // part) * ((capacity + LANES - 1) // LANES) + s // LANES) * part * LANES + j * LANES
        copy_rows(n, 16, lambda t, base=base: pos_ref[base + t], table, rows, s)
    n = fill_ref[(first + j) * LANES]
    live = iota((capacity, 1), 0) < n
    xb = jnp.where(live, rows[:, 0, :], 0)
    gb = jnp.where(live, rows[:, 1, :], 0)
    nt = (((1,), (1,)), ((), ()))
    tn = (((0,), (0,)), ((), ()))
    out = back = None
    for f in range(0, w_in_ref.shape[2], f_tile):
        span = slice(f, f + f_tile)
        a = jnp.dot(xb, w_in_ref[0, :, span], preferred_element_type=F32)
        dh = lax.dot_general(gb, w_out_ref[0, span, :], nt, preferred_element_type=F32).astype(BF16).astype(F32)
        a2 = a * a
        th = jnp.tanh(a * (GELU_C + (GELU_C * GELU_A) * a2))
        cdf = 0.5 + 0.5 * th
        h = (a * cdf).astype(BF16)
        slope = cdf + (0.5 * a) * (1.0 - th * th) * (GELU_C + (3.0 * GELU_C * GELU_A) * a2)
        da = (dh * slope).astype(BF16)
        o = jnp.dot(h, w_out_ref[0, span, :], preferred_element_type=F32)
        d = lax.dot_general(da, w_in_ref[0, :, span], nt, preferred_element_type=F32)
        out = o if out is None else out + o
        back = d if back is None else back + d
        gw_out_ref[0, span, :] = lax.dot_general(h, gb, tn, preferred_element_type=F32).astype(BF16)
        gw_in_ref[0, :, span] = lax.dot_general(xb, da, tn, preferred_element_type=F32).astype(BF16)
    out_ref[:, 0, :] = out.astype(BF16)
    out_ref[:, 1, :] = back.astype(BF16)


def combine_kernel(tile, n_tables, pos_ref, x_ref, gate_ref, dy_ref, *refs):
    pieces = refs[:n_tables]
    y_ref, dx_ref, dgate_ref, table, rows, sems = refs[n_tables:]
    step = pl.program_id(0)

    @pl.when(step == 0)
    def _():
        table[pl.ds(table.shape[0] - 8, 8)] = jnp.zeros((8,) + table.shape[1:], BF16)
        load_tables(pieces, table, sems)

    copy_rows(tile, 16, lambda t: pos_ref[step * tile + t], table, rows)
    width = x_ref.shape[1]
    for q in range(tile // LANES):
        block = pl.ds(q * LANES, LANES)
        at = pl.ds(step * (tile // LANES) + q, 1)
        gate = column(gate_ref[at, :])
        gate = jnp.concatenate([gate] * (width // LANES), axis=1)
        o = rows[block, 0, :].astype(F32)
        d = rows[block, 1, :].astype(F32)
        dy = dy_ref[block, :].astype(F32)
        y_ref[block, :] = (x_ref[block, :].astype(F32) + gate * o).astype(BF16)
        dx_ref[block, :] = (dy + d).astype(BF16)
        prod = dy * o
        part = prod[:, 0:LANES]
        for k in range(LANES, width, LANES):
            part = part + prod[:, k:k + LANES]
        dgate_ref[at, :] = jnp.sum(jnp.transpose(part), axis=0, keepdims=True)


def params():
    return pltpu.CompilerParams(vmem_limit_bytes=BIG)


def list_pass(groups, half, x_in, gate, grad_y, w_in, w_out, idx2, rank, every, own_rows, sib_rows):
    sds = jax.ShapeDtypeStruct
    n_tokens, d_model = x_in.shape
    local_experts, _, d_ff = w_in.shape
    chips = groups // CORES
    capacity = (CAP_NUM * n_tokens) // (CAP_DEN * local_experts)
    part = local_experts // CHUNKS
    slot_rows = (capacity + LANES - 1) // LANES
    lists = (chips - 1) * half
    region = lists + slot_rows * part * LANES
    n_high = (CHUNKS * region // LANES + 7) // 8 * 8
    token_rows = n_tokens // LANES
    row = (2, d_model)
    list_shape = sds((half,) + row, BF16)

    def to_chip(v, m):
        return lax.ppermute(v, 'expert', [(i, i ^ (CORES * m)) for i in range(groups)])

    def to_sibling(v):
        return lax.ppermute(v, 'expert', [(i, i ^ 1) for i in range(groups)])

    inv, recv, ret, fpos, fill = pl.pallas_call(
        functools.partial(map_kernel, capacity, local_experts, half),
        out_shape=[sds((n_high, LANES), I32), sds((CHUNKS * slot_rows * part, LANES), I32), sds((CHUNKS * (chips - 1), half), I32),
                   sds((token_rows, LANES), I32), sds((local_experts, LANES), I32)],
        in_specs=[VMEM] * 3, out_specs=[VMEM] * 5,
        scratch_shapes=[pltpu.VMEM((LANES, LANES), I32), pltpu.VMEM((CORES * token_rows, LANES), I32)],
        compiler_params=params(), name='maps',
    )(idx2, rank, every)
    inv, recv, ret, fpos, fill = [v.reshape(-1) for v in (inv, recv, ret, fpos, fill)]

    def pick(tables, index, first, name):
        n = sum(t.shape[0] for t in tables)
        return pl.pallas_call(
            functools.partial(pick_kernel, len(tables), first),
            out_shape=[list_shape] * (chips - 1),
            in_specs=[SMEM] + [ANY] * len(tables), out_specs=[VMEM] * (chips - 1),
            scratch_shapes=[pltpu.VMEM((n,) + row, BF16), pltpu.SemaphoreType.DMA((len(tables),))],
            cost_estimate=pl.CostEstimate(flops=20 * 10 ** 6, bytes_accessed=2 * n * 4 * d_model, transcendentals=0),
            compiler_params=params(), name=name,
        )(index, *tables)

    arrived = []
    for c in range(CHUNKS):
        sent = pick([own_rows, sib_rows], inv, c * region, 'pick')
        got = [to_chip(v, m + 1) for m, v in enumerate(sent)]
        arrived.append(got + [to_sibling(v) for v in got])
    grads = []
    final = []
    for c in range(CHUNKS):
        first = c * part
        weight_in = pl.BlockSpec((1, d_model, d_ff), lambda i, first=first: (first + i, 0, 0))
        weight_out = pl.BlockSpec((1, d_ff, d_model), lambda i, first=first: (first + i, 0, 0))
        row_block = pl.BlockSpec((capacity,) + row, lambda i: (i, 0, 0))
        tables = arrived[c] + [own_rows, sib_rows]
        n = len(tables)
        out_rows, *grads = pl.pallas_call(
            functools.partial(expert_kernel, n, len(grads), first, part, capacity, 512),
            grid=(part,),
            out_shape=[sds((part * capacity,) + row, BF16), sds(w_in.shape, BF16), sds(w_out.shape, BF16)],
            in_specs=[SMEM, SMEM, weight_in, weight_out] + [ANY] * (n + len(grads)),
            out_specs=[row_block, weight_in, weight_out],
            input_output_aliases={4 + n: 1, 5 + n: 2} if grads else {},
            scratch_shapes=[pltpu.VMEM((sum(t.shape[0] for t in tables),) + row, BF16), pltpu.VMEM((capacity,) + row, BF16), pltpu.SemaphoreType.DMA((n,))],
            compiler_params=params(),
            cost_estimate=pl.CostEstimate(flops=12 * part * capacity * d_model * d_ff, bytes_accessed=8 * part * d_model * d_ff, transcendentals=part * capacity * d_ff),
            name='experts',
        )(fill, recv, w_in, w_out, *tables, *grads)
        sib_out = to_sibling(out_rows)
        sent = pick([out_rows, sib_out], ret, c * lists, 'pack')
        got = [to_chip(v, m + 1) for m, v in enumerate(sent)]
        final += got + [to_sibling(v) for v in got] + [out_rows, sib_out]
    tile = 256
    wide = pl.BlockSpec((tile, d_model), lambda i: (i, 0))
    y_out, grad_x, grad_gate = pl.pallas_call(
        functools.partial(combine_kernel, tile, len(final)),
        grid=(n_tokens // tile,),
        out_shape=[sds(x_in.shape, BF16), sds(x_in.shape, BF16), sds((token_rows, LANES), F32)],
        in_specs=[SMEM, wide, VMEM, wide] + [ANY] * len(final),
        out_specs=[wide, wide, VMEM],
        scratch_shapes=[pltpu.VMEM((sum(t.shape[0] for t in final) + 8,) + row, BF16), pltpu.VMEM((tile,) + row, BF16), pltpu.SemaphoreType.DMA((len(final),))],
        compiler_params=params(), name='combine',
    )(fpos, x_in, gate, grad_y, *final)
    return y_out, grad_x, grad_gate.reshape(n_tokens, 1), grads[0], grads[1]


def solution(mesh):
    groups = mesh.shape['expert']
    tok_spec = P(('data', 'expert'), None)
    weight_spec = P('expert', None, None)
    grad_spec = P(('data', 'expert'), None, None)

    def device_pass(x_in, expert_idx, gate_weight, grad_y, w_in, w_out):
        sds = jax.ShapeDtypeStruct
        n_tokens, d_model = x_in.shape
        local_experts = w_in.shape[0]
        capacity = (CAP_NUM * n_tokens) // (CAP_DEN * local_experts)
        token_rows = n_tokens // LANES
        sibling = [(i, i ^ 1) for i in range(groups)]
        idx = expert_idx.reshape(token_rows, LANES)
        gate = gate_weight.reshape(token_rows, LANES)
        core = lax.rem(lax.axis_index('expert'), CORES)
        other = lax.ppermute(idx, 'expert', sibling)
        idx2 = jnp.where(core == 0, jnp.concatenate([idx, other]), jnp.concatenate([other, idx]))
        tile = 256
        wide = pl.BlockSpec((tile, d_model), lambda i: (i, 0))
        own_rows = pl.pallas_call(
            functools.partial(build_kernel, tile),
            grid=(n_tokens // tile,),
            out_shape=sds((n_tokens, 2, d_model), BF16),
            in_specs=[wide, VMEM, wide],
            out_specs=pl.BlockSpec((tile, 2, d_model), lambda i: (i, 0, 0)),
            compiler_params=params(), name='build',
        )(x_in, gate, grad_y)
        sib_rows = lax.ppermute(own_rows, 'expert', sibling)
        rank, every = pl.pallas_call(
            functools.partial(count_kernel, groups),
            out_shape=[sds((CORES * token_rows, LANES), I32), sds((groups, LANES), I32)],
            in_specs=[VMEM], out_specs=[VMEM] * 2,
            scratch_shapes=[pltpu.VMEM((8, LANES), I32), pltpu.VMEM((groups, 8, LANES), I32),
                            pltpu.SemaphoreType.DMA((groups,)), pltpu.SemaphoreType.DMA((groups,))],
            cost_estimate=pl.CostEstimate(flops=20 * 10 ** 6, bytes_accessed=10 ** 6, transcendentals=0),
            compiler_params=pltpu.CompilerParams(collective_id=0, has_side_effects=True), name='count',
        )(idx2)
        need = pl.pallas_call(
            functools.partial(need_kernel, capacity, local_experts),
            out_shape=sds((1, LANES), I32), in_specs=[VMEM], out_specs=VMEM, name='need',
        )(every)[0, 0]
        branches = [lambda *a, half=half: list_pass(groups, half, *a[:2], *a[3:]) for half in HALVES]
        branches.append(lambda x, g, i, dy, wi, wo, *rest: padded_pass(groups, x, i, g.reshape(n_tokens, 1), dy, wi, wo))
        which = sum((need > 2 * half).astype(I32) for half in HALVES)
        return lax.switch(which, branches, x_in, gate, expert_idx, grad_y, w_in, w_out, idx2, rank, every, own_rows, sib_rows)

    return jax.shard_map(device_pass, mesh=mesh,
                         in_specs=(tok_spec, tok_spec, tok_spec, tok_spec, weight_spec, weight_spec),
                         out_specs=(tok_spec, tok_spec, tok_spec, grad_spec, grad_spec), check_vma=False)
```

```python
import functools

import jax
import jax.numpy as jnp
from jax import lax
from jax.experimental import pallas as pl
from jax.experimental.pallas import tpu as pltpu
from jax.sharding import PartitionSpec as P


CAP_NUM = 5
CAP_DEN = 4
PAIR_FACTOR = 2
CHUNKS = 2
HALVES = (768, 1024)
CORES = 2
LANES = 128
BIG = 60 * 2 ** 20
F32 = jnp.float32
BF16 = jnp.bfloat16
I32 = jnp.int32
GELU_C = 0.7978845608028654
GELU_A = 0.044715
VMEM = pl.BlockSpec(memory_space=pltpu.VMEM)
SMEM = pl.BlockSpec(memory_space=pltpu.SMEM)
ANY = pl.BlockSpec(memory_space=pl.ANY)


def local_ranks(flat_idx, num_experts):
    one_hot = (flat_idx[:, None] == jnp.arange(num_experts, dtype=jnp.int32)[None, :]).astype(jnp.int32)
    running = jnp.cumsum(one_hot, axis=0)
    return jnp.sum((running - one_hot) * one_hot, axis=1), running[-1]


def exchange_maps(flat_idx, local_rank, counts_all, my_index, local_experts, capacity, pair_cap):
    groups, num_experts = counts_all.shape
    n_pairs = flat_idx.shape[0]
    through = jnp.cumsum(counts_all, axis=0)
    before = through - counts_all
    kept_all = jnp.clip(capacity - before, 0, counts_all)
    before_mine = lax.dynamic_index_in_dim(before, my_index, 0, keepdims=False)
    kept_grid = lax.dynamic_index_in_dim(kept_all, my_index, 0, keepdims=False).reshape(groups, local_experts)
    send_start = (jnp.cumsum(kept_grid, axis=1) - kept_grid).reshape(num_experts)
    pair_slot = before_mine[flat_idx] + local_rank
    target = jnp.where(pair_slot < capacity, (flat_idx // local_experts) * pair_cap + send_start[flat_idx] + local_rank, groups * pair_cap)
    send_src = jnp.full((groups * pair_cap,), n_pairs, jnp.int32).at[target].set(jnp.arange(n_pairs, dtype=jnp.int32), mode='drop')
    first_expert = my_index * local_experts
    through_own = lax.dynamic_slice_in_dim(through, first_expert, local_experts, axis=1)
    before_own = lax.dynamic_slice_in_dim(before, first_expert, local_experts, axis=1)
    kept_own = lax.dynamic_slice_in_dim(kept_all, first_expert, local_experts, axis=1)
    start_own = jnp.cumsum(kept_own, axis=1) - kept_own
    slot_ids = jnp.arange(capacity, dtype=jnp.int32)
    source_dev = jnp.sum((through_own.T[:, None, :] <= slot_ids[None, :, None]).astype(jnp.int32), axis=2)
    filled = slot_ids[None, :] < jnp.minimum(through_own[-1], capacity)[:, None]
    source_dev = jnp.minimum(source_dev, groups - 1)
    start_at = jnp.take_along_axis(start_own.T, source_dev, axis=1)
    before_at = jnp.take_along_axis(before_own.T, source_dev, axis=1)
    recv_pos = jnp.where(filled, source_dev * pair_cap + start_at + slot_ids[None, :] - before_at, groups * pair_cap).reshape(local_experts * capacity)
    back_src = jnp.full((groups * pair_cap,), local_experts * capacity, jnp.int32).at[recv_pos].set(jnp.arange(local_experts * capacity, dtype=jnp.int32), mode='drop')
    return target, send_src, recv_pos, back_src


def exchange(rows):
    return lax.all_to_all(rows, 'expert', 0, 0, tiled=True)


def gather_rows(table, positions):
    return jnp.take(table, positions, axis=0, mode='fill', fill_value=0)


def padded_pass(groups, x_in, expert_idx, gate_weight, grad_y, w_in, w_out):
    n_tokens, top_k = expert_idx.shape
    local_experts, d_model = w_in.shape[0], w_in.shape[1]
    num_experts = local_experts * groups
    n_pairs = n_tokens * top_k
    capacity = (CAP_NUM * n_pairs * groups) // (CAP_DEN * num_experts)
    pair_cap = PAIR_FACTOR * n_pairs // groups
    my_index = lax.axis_index('expert')
    flat_idx = expert_idx.reshape(n_pairs)
    local_rank, counts = local_ranks(flat_idx, num_experts)
    counts_all = lax.all_gather(counts, 'expert')
    target, send_src, recv_pos, back_src = exchange_maps(flat_idx, local_rank, counts_all, my_index, local_experts, capacity, pair_cap)
    exp_rows = gather_rows(exchange(gather_rows(x_in, send_src // top_k)), recv_pos).reshape(local_experts, capacity, d_model)
    pre_act = jnp.einsum('lcd,ldf->lcf', exp_rows, w_in, preferred_element_type=jnp.float32)
    act_full, gelu_pull = jax.vjp(jax.nn.gelu, pre_act)
    act_bf = act_full.astype(jnp.bfloat16)
    out_rows = jnp.einsum('lcf,lfd->lcd', act_bf, w_out, preferred_element_type=jnp.float32).astype(jnp.bfloat16)
    back_out = gather_rows(out_rows.reshape(local_experts * capacity, d_model), back_src)
    out_pair = gather_rows(exchange(back_out), target).reshape(n_tokens, top_k, d_model)
    y_out = (x_in.astype(jnp.float32) + jnp.sum(gate_weight[:, :, None] * out_pair, axis=1)).astype(jnp.bfloat16)
    grad_gate = jnp.einsum('tkd,td->tk', out_pair, grad_y, preferred_element_type=jnp.float32)
    scaled_grad = (gate_weight[:, :, None] * grad_y[:, None, :]).astype(jnp.bfloat16).reshape(n_pairs, d_model)
    grad_rows = gather_rows(exchange(gather_rows(scaled_grad, send_src)), recv_pos).reshape(local_experts, capacity, d_model)
    grad_act = jnp.einsum('lcd,lfd->lcf', grad_rows, w_out, preferred_element_type=jnp.float32).astype(jnp.bfloat16)
    grad_pre = gelu_pull(grad_act.astype(jnp.float32))[0].astype(jnp.bfloat16)
    grad_w_out = jnp.einsum('lcf,lcd->lfd', act_bf, grad_rows, preferred_element_type=jnp.float32).astype(jnp.bfloat16)
    grad_w_in = jnp.einsum('lcd,lcf->ldf', exp_rows, grad_pre, preferred_element_type=jnp.float32).astype(jnp.bfloat16)
    grad_in_rows = jnp.einsum('lcf,ldf->lcd', grad_pre, w_in, preferred_element_type=jnp.float32).astype(jnp.bfloat16)
    back_grad = gather_rows(grad_in_rows.reshape(local_experts * capacity, d_model), back_src)
    grad_pair = gather_rows(exchange(back_grad), target).reshape(n_tokens, top_k, d_model)
    grad_x = (grad_y.astype(jnp.float32) + jnp.sum(grad_pair, axis=1, dtype=jnp.float32)).astype(jnp.bfloat16)
    return y_out, grad_x, grad_gate, grad_w_in, grad_w_out


def iota(shape, dim):
    return lax.broadcasted_iota(jnp.int32, shape, dim)


def exact_dot(a, b):
    return jnp.dot(a, b, preferred_element_type=F32, precision=lax.Precision.HIGHEST)


def xor_chip(a, b):
    return lax.rem(lax.div(a, 2) + lax.div(b, 2), 2) * 2 + lax.rem(lax.rem(a, 2) + lax.rem(b, 2), 2)


def sum_rows(m):
    return jnp.sum(m, axis=0, keepdims=True)


def count_kernel(groups, idx_ref, rank_ref, every_ref, mine, every, send_sem, recv_sem):
    me = lax.axis_index('expert')
    core = lax.rem(me, CORES)
    rows = idx_ref.shape[0] // CORES
    barrier = pltpu.get_barrier_semaphore()
    for s in range(1, groups):
        pl.semaphore_signal(barrier, inc=1, device_id={'expert': lax.rem(me + s, groups)}, device_id_type=pl.DeviceIdType.MESH)

    def one_hot(r):
        return jnp.where(iota((LANES, LANES), 0) == idx_ref[pl.ds(r, 1), :], 1.0, 0.0)

    seen = jnp.zeros((LANES, LANES), F32)
    for r in range(rows):
        seen = seen + one_hot(core * rows + r)
    counts = lax.dot_general(jnp.ones((8, LANES), BF16), seen.astype(BF16), (((1,), (1,)), ((), ())), preferred_element_type=F32)
    mine[...] = counts.astype(I32)
    every[pl.ds(me, 1)] = counts.astype(I32)[None]
    pl.semaphore_wait(barrier, groups - 1)
    copies = []
    for s in range(1, groups):
        copy = pltpu.make_async_remote_copy(src_ref=mine, dst_ref=every.at[me], send_sem=send_sem.at[s], recv_sem=recv_sem.at[s],
                                            device_id={'expert': lax.rem(me + s, groups)}, device_id_type=pl.DeviceIdType.MESH)
        copy.start()
        copies.append(copy)
    earlier = jnp.where(iota((LANES, LANES), 0) < iota((LANES, LANES), 1), 1.0, 0.0)
    mix = jnp.concatenate([earlier, jnp.ones((LANES, LANES), F32)], axis=0).astype(BF16)
    done = jnp.zeros((LANES, LANES), F32)
    for r in range(rows * CORES):
        hot = one_hot(r)
        rank = jnp.dot(jnp.concatenate([hot, done], axis=1).astype(BF16), mix, preferred_element_type=F32)
        rank_ref[r:r + 1, :] = sum_rows(hot * rank).astype(I32)
        done = done + hot
    for copy in copies:
        copy.wait()
    every_ref[...] = every[:, 0, :]


def chip_tables(cnt, capacity, local_experts):
    groups = cnt.shape[0]
    part = local_experts // CHUNKS
    source = iota((groups, LANES), 0)
    before = jnp.zeros((groups, LANES), F32)
    for i in range(groups - 1):
        before = before + jnp.where(source > i, cnt[i:i + 1, :], 0.0)
    kept = jnp.clip(capacity - before, 0.0, cnt)
    chips = groups // CORES
    k2 = jnp.concatenate([kept[CORES * c:CORES * c + 1] + kept[CORES * c + 1:CORES * c + 2] for c in range(chips)], axis=0)
    b0 = jnp.concatenate([before[CORES * c:CORES * c + 1] for c in range(chips)], axis=0)
    e0, e1 = iota((LANES, LANES), 0), iota((LANES, LANES), 1)
    chip_experts = CORES * local_experts
    same = (lax.div(e0, chip_experts) == lax.div(e1, chip_experts)) & (lax.rem(lax.div(e0, part), CHUNKS) == lax.rem(lax.div(e1, part), CHUNKS))
    start = exact_dot(jnp.concatenate([k2, k2], axis=0), jnp.where(same & (e0 < e1), 1.0, 0.0))[:chips]
    return k2, b0, start


def need_kernel(capacity, local_experts, every_ref, need_ref):
    k2, _, start = chip_tables(every_ref[...].astype(F32), capacity, local_experts)
    away = iota(k2.shape, 0) != lax.div(iota(k2.shape, 1), CORES * local_experts)
    longest = jnp.max(jnp.where(away, start + k2, 0.0), axis=0, keepdims=True)
    need_ref[...] = jnp.broadcast_to(jnp.max(longest, axis=1, keepdims=True), (1, LANES)).astype(I32)


def map_kernel(capacity, local_experts, half, idx_ref, rank_ref, every_ref, inv_ref, recv_ref, ret_ref, fpos_ref, fill_ref, cols, fall):
    me = lax.axis_index('expert')
    core, chip = lax.rem(me, CORES), lax.div(me, CORES)
    rows = idx_ref.shape[0] // CORES
    part = local_experts // CHUNKS
    k2, b0, start = chip_tables(every_ref[...].astype(F32), capacity, local_experts)
    chips = k2.shape[0]
    mine = iota(k2.shape, 0) == chip
    pad = jnp.zeros((LANES - 3 * chips, LANES), F32)
    cols[...] = jnp.transpose(jnp.concatenate([k2, b0, start, pad], axis=0)).astype(I32)
    look = jnp.concatenate([sum_rows(jnp.where(mine, v, 0.0)) for v in (k2, b0, start)], axis=0)
    high = jnp.floor(look * (1.0 / LANES))
    look = jnp.concatenate([high, look - LANES * high, jnp.zeros((2, LANES), F32)], axis=0).astype(BF16)
    part_rows = part * capacity
    slot_rows = (capacity + LANES - 1) // LANES
    region = (chips - 1) * half + slot_rows * part * LANES
    final = 2 * (chips - 1) * half + CORES * part_rows
    n_high = (CHUNKS * region // LANES + 7) // 8 * 8
    acc = jnp.zeros((2 * n_high, LANES), F32)
    lane = iota((1, LANES), 1)
    nt = (((1,), (1,)), ((), ()))
    for r in range(rows * CORES):
        e = idx_ref[r:r + 1, :]
        hot = jnp.where(iota((LANES, LANES), 0) == e, 1.0, 0.0).astype(BF16)
        found = jnp.dot(look, hot, preferred_element_type=F32).astype(I32)
        found = found[0:3] * LANES + found[3:6]
        rank = rank_ref[r:r + 1, :]
        slot = found[1:2] + rank
        q = found[2:3] + rank
        owner = lax.div(e, local_experts)
        group = lax.rem(lax.div(e, part), CHUNKS)
        el = lax.rem(e, part)
        m = xor_chip(lax.div(owner, CORES), chip)
        here = q - core * half
        slot_at = (chips - 1) * half + lax.div(slot, LANES) * (part * LANES) + el * LANES + lax.rem(slot, LANES)
        pos = group * region + jnp.where(m > 0, (m - 1) * half + here, slot_at)
        kept = rank < found[0:1]
        in_half = (here >= 0) & (here < half)
        valid = kept & (((m > 0) & in_half) | ((m == 0) & (owner == me)))
        pos = jnp.where(valid, pos, -1)
        hi = jnp.where(iota((n_high, LANES), 0) == jnp.where(valid, lax.div(pos, LANES), -1), 1.0, 0.0)
        lo = jnp.where(iota((LANES, LANES), 0) == lax.rem(pos, LANES), 1.0, 0.0).astype(BF16)
        row_id = (r % rows + jnp.where(core == r // rows, 0, rows)).astype(F32)
        left = jnp.concatenate([hi * row_id, hi * lane.astype(F32)], axis=0).astype(BF16)
        acc = acc + lax.dot_general(left, lo, nt, preferred_element_type=F32)
        other = (chips - 1) * half
        in_list = jnp.where(in_half, 0, other) + (m - 1) * half + lax.rem(q, half)
        in_own = 2 * other + jnp.where(owner == me, 0, part_rows) + el * capacity + slot
        fall[r:r + 1, :] = jnp.where(kept, group * final + jnp.where(m > 0, in_list, in_own), CHUNKS * final)
    fpos_ref[...] = fall[pl.ds(core * rows, rows), :]
    inv = (acc[:n_high] * LANES + acc[n_high:]).astype(I32)
    inv_ref[...] = inv
    lists = (chips - 1) * half
    for c in range(CHUNKS):
        col = cols[pl.ds(me * local_experts + c * part, part), :]
        total = col[:, 0:1]
        for i in range(1, chips):
            total = total + col[:, i:i + 1]
        fill_ref[c * part:(c + 1) * part, :] = jnp.broadcast_to(total, (part, LANES))
        for j in range(slot_rows):
            s = j * LANES + iota((part, LANES), 1)
            first = (c * region + lists) // LANES + j * part
            at = jnp.zeros((part, LANES), I32)
            for src in range(chips):
                rel = s - col[:, chips + src:chips + src + 1]
                q = col[:, 2 * chips + src:2 * chips + src + 1] + rel
                here = q - core * half
                away = xor_chip(src, chip)
                remote = jnp.where((here >= 0) & (here < half), 0, lists) + (away - 1) * half + lax.rem(jnp.maximum(q, 0), half)
                own = 2 * lists + inv[first:first + part]
                at = jnp.where((rel >= 0) & (rel < col[:, src:src + 1]), jnp.where(away > 0, remote, own), at)
            row = (c * slot_rows + j) * part
            recv_ref[row:row + part, :] = at
        q = core * half + iota((part, half), 1)
        for m in range(1, chips):
            src = xor_chip(m, chip)
            at = jnp.zeros((1, half), I32)
            for o in range(CORES):
                col = cols[pl.ds((chip * CORES + o) * local_experts + c * part, part), :]

                def pick(base):
                    return jnp.sum(jnp.where(iota((part, LANES), 1) == base + src, col, 0), axis=1, keepdims=True)

                rel = q - pick(2 * chips)
                base = jnp.where(core == o, 0, part_rows) + iota((part, 1), 0) * capacity
                hit = (rel >= 0) & (rel < pick(0))
                at = at + sum_rows(jnp.where(hit, base + rel + pick(chips), 0))
            ret_ref[c * (chips - 1) + m - 1:c * (chips - 1) + m, :] = at


def column(row):
    return jnp.transpose(jnp.broadcast_to(row, (LANES, LANES)))


def build_kernel(tile, x_ref, gate_ref, dy_ref, out_ref):
    step = pl.program_id(0)
    for q in range(tile // LANES):
        block = pl.ds(q * LANES, LANES)
        gate = column(gate_ref[pl.ds(step * (tile // LANES) + q, 1), :])
        gate = jnp.concatenate([gate] * (x_ref.shape[1] // LANES), axis=1)
        out_ref[block, 0, :] = x_ref[block, :]
        out_ref[block, 1, :] = (gate * dy_ref[block, :].astype(F32)).astype(BF16)


def copy_rows(n, unroll, index, table, rows, first=0):
    def body(b, carry):
        for u in range(unroll):
            rows[pl.ds(first + b * unroll + u, 1)] = table[pl.ds(index(b * unroll + u), 1)]
        return carry

    lax.fori_loop(0, n // unroll, body, 0)


def load_tables(pieces, table, sems):
    at = 0
    copies = []
    for i, piece in enumerate(pieces):
        copy = pltpu.make_async_copy(piece, table.at[pl.ds(at, piece.shape[0])], sems.at[i])
        copy.start()
        copies.append(copy)
        at += piece.shape[0]
    for copy in copies:
        copy.wait()


def pick_kernel(n_tables, first, pos_ref, *refs):
    pieces, outs, (table, sems) = refs[:n_tables], refs[n_tables:-2], refs[-2:]
    load_tables(pieces, table, sems)
    at = first
    for out in outs:
        copy_rows(out.shape[0], 16, lambda t, at=at: pos_ref[at + t], table, out)
        at += out.shape[0]


def expert_kernel(n_tables, n_extra, first, part, capacity, f_tile, fill_ref, pos_ref, w_in_ref, w_out_ref, *refs):
    pieces = refs[:n_tables]
    out_ref, gw_in_ref, gw_out_ref, table, rows, sems = refs[n_tables + n_extra:]
    j = pl.program_id(0)

    @pl.when(j == 0)
    def _():
        load_tables(pieces, table, sems)

    for s in range(0, capacity, LANES):
        n = min(LANES, capacity - s)
        base = ((first // part) * ((capacity + LANES - 1) // LANES) + s // LANES) * part * LANES + j * LANES
        copy_rows(n, 16, lambda t, base=base: pos_ref[base + t], table, rows, s)
    n = fill_ref[(first + j) * LANES]
    live = iota((capacity, 1), 0) < n
    xb = jnp.where(live, rows[:, 0, :], 0)
    gb = jnp.where(live, rows[:, 1, :], 0)
    nt = (((1,), (1,)), ((), ()))
    tn = (((0,), (0,)), ((), ()))
    out = back = None
    for f in range(0, w_in_ref.shape[2], f_tile):
        span = slice(f, f + f_tile)
        a = jnp.dot(xb, w_in_ref[0, :, span], preferred_element_type=F32)
        dh = lax.dot_general(gb, w_out_ref[0, span, :], nt, preferred_element_type=F32).astype(BF16).astype(F32)
        a2 = a * a
        th = jnp.tanh(a * (GELU_C + (GELU_C * GELU_A) * a2))
        cdf = 0.5 + 0.5 * th
        h = (a * cdf).astype(BF16)
        slope = cdf + (0.5 * a) * (1.0 - th * th) * (GELU_C + (3.0 * GELU_C * GELU_A) * a2)
        da = (dh * slope).astype(BF16)
        o = jnp.dot(h, w_out_ref[0, span, :], preferred_element_type=F32)
        d = lax.dot_general(da, w_in_ref[0, :, span], nt, preferred_element_type=F32)
        out = o if out is None else out + o
        back = d if back is None else back + d
        gw_out_ref[0, span, :] = lax.dot_general(h, gb, tn, preferred_element_type=F32).astype(BF16)
        gw_in_ref[0, :, span] = lax.dot_general(xb, da, tn, preferred_element_type=F32).astype(BF16)
    out_ref[:, 0, :] = out.astype(BF16)
    out_ref[:, 1, :] = back.astype(BF16)


def combine_kernel(tile, n_tables, pos_ref, x_ref, gate_ref, dy_ref, *refs):
    pieces = refs[:n_tables]
    y_ref, dx_ref, dgate_ref, table, rows, sems = refs[n_tables:]
    step = pl.program_id(0)

    @pl.when(step == 0)
    def _():
        table[pl.ds(table.shape[0] - 8, 8)] = jnp.zeros((8,) + table.shape[1:], BF16)
        load_tables(pieces, table, sems)

    copy_rows(tile, 16, lambda t: pos_ref[step * tile + t], table, rows)
    width = x_ref.shape[1]
    for q in range(tile // LANES):
        block = pl.ds(q * LANES, LANES)
        at = pl.ds(step * (tile // LANES) + q, 1)
        gate = column(gate_ref[at, :])
        gate = jnp.concatenate([gate] * (width // LANES), axis=1)
        o = rows[block, 0, :].astype(F32)
        d = rows[block, 1, :].astype(F32)
        dy = dy_ref[block, :].astype(F32)
        y_ref[block, :] = (x_ref[block, :].astype(F32) + gate * o).astype(BF16)
        dx_ref[block, :] = (dy + d).astype(BF16)
        prod = dy * o
        part = prod[:, 0:LANES]
        for k in range(LANES, width, LANES):
            part = part + prod[:, k:k + LANES]
        dgate_ref[at, :] = jnp.sum(jnp.transpose(part), axis=0, keepdims=True)


def params():
    return pltpu.CompilerParams(vmem_limit_bytes=BIG)


def list_pass(groups, half, x_in, gate, grad_y, w_in, w_out, idx2, rank, every, own_rows):
    sds = jax.ShapeDtypeStruct
    n_tokens, d_model = x_in.shape
    local_experts, _, d_ff = w_in.shape
    chips = groups // CORES
    capacity = (CAP_NUM * n_tokens) // (CAP_DEN * local_experts)
    part = local_experts // CHUNKS
    slot_rows = (capacity + LANES - 1) // LANES
    lists = (chips - 1) * half
    region = lists + slot_rows * part * LANES
    n_high = (CHUNKS * region // LANES + 7) // 8 * 8
    token_rows = n_tokens // LANES
    row = (2, d_model)
    list_shape = sds((half,) + row, BF16)

    def to_chip(v, m):
        return lax.ppermute(v, 'expert', [(i, i ^ (CORES * m)) for i in range(groups)])

    def to_sibling(v):
        return lax.ppermute(v, 'expert', [(i, i ^ 1) for i in range(groups)])

    sib_rows = to_sibling(own_rows)
    inv, recv, ret, fpos, fill = pl.pallas_call(
        functools.partial(map_kernel, capacity, local_experts, half),
        out_shape=[sds((n_high, LANES), I32), sds((CHUNKS * slot_rows * part, LANES), I32), sds((CHUNKS * (chips - 1), half), I32),
                   sds((token_rows, LANES), I32), sds((local_experts, LANES), I32)],
        in_specs=[VMEM] * 3, out_specs=[VMEM] * 5,
        scratch_shapes=[pltpu.VMEM((LANES, LANES), I32), pltpu.VMEM((CORES * token_rows, LANES), I32)],
        compiler_params=params(), name='maps',
        cost_estimate=pl.CostEstimate(flops=40 * 10 ** 6, bytes_accessed=10 ** 6, transcendentals=0),
    )(idx2, rank, every)
    inv, recv, ret, fpos, fill = [v.reshape(-1) for v in (inv, recv, ret, fpos, fill)]

    def pick(tables, index, first):
        n = sum(t.shape[0] for t in tables)
        return pl.pallas_call(
            functools.partial(pick_kernel, len(tables), first),
            out_shape=[list_shape] * (chips - 1),
            in_specs=[SMEM] + [ANY] * len(tables), out_specs=[VMEM] * (chips - 1),
            scratch_shapes=[pltpu.VMEM((n,) + row, BF16), pltpu.SemaphoreType.DMA((len(tables),))],
            cost_estimate=pl.CostEstimate(flops=20 * 10 ** 6, bytes_accessed=2 * n * 4 * d_model, transcendentals=0),
            compiler_params=params(),
        )(index, *tables)

    arrived = []
    for c in range(CHUNKS):
        sent = pick([own_rows, sib_rows], inv, c * region)
        got = [to_chip(v, m + 1) for m, v in enumerate(sent)]
        arrived.append(got + [to_sibling(v) for v in got])
    grads = []
    final = []
    for c in range(CHUNKS):
        first = c * part
        weight_in = pl.BlockSpec((1, d_model, d_ff), lambda i, first=first: (first + i, 0, 0))
        weight_out = pl.BlockSpec((1, d_ff, d_model), lambda i, first=first: (first + i, 0, 0))
        row_block = pl.BlockSpec((capacity,) + row, lambda i: (i, 0, 0))
        tables = arrived[c] + [own_rows, sib_rows]
        n = len(tables)
        experts = pl.pallas_call(
            functools.partial(expert_kernel, n, len(grads), first, part, capacity, 512),
            grid=(part,),
            out_shape=[sds((part * capacity,) + row, BF16), sds(w_in.shape, BF16), sds(w_out.shape, BF16)],
            in_specs=[SMEM, SMEM, weight_in, weight_out] + [ANY] * (n + len(grads)),
            out_specs=[row_block, weight_in, weight_out],
            input_output_aliases={4 + n: 1, 5 + n: 2} if grads else {},
            scratch_shapes=[pltpu.VMEM((sum(t.shape[0] for t in tables),) + row, BF16), pltpu.VMEM((capacity,) + row, BF16), pltpu.SemaphoreType.DMA((n,))],
            compiler_params=params(),
            cost_estimate=pl.CostEstimate(flops=12 * part * capacity * d_model * d_ff, bytes_accessed=8 * part * d_model * d_ff, transcendentals=part * capacity * d_ff),
            name='experts',
        )
        out_rows, *grads = experts(fill, recv, w_in, w_out, *tables, *grads)
        sib_out = to_sibling(out_rows)
        sent = pick([out_rows, sib_out], ret, c * lists)
        got = [to_chip(v, m + 1) for m, v in enumerate(sent)]
        final += got + [to_sibling(v) for v in got] + [out_rows, sib_out]
    tile = 256
    wide = pl.BlockSpec((tile, d_model), lambda i: (i, 0))
    y_out, grad_x, grad_gate = pl.pallas_call(
        functools.partial(combine_kernel, tile, len(final)),
        grid=(n_tokens // tile,),
        out_shape=[sds(x_in.shape, BF16), sds(x_in.shape, BF16), sds((token_rows, LANES), F32)],
        in_specs=[SMEM, wide, VMEM, wide] + [ANY] * len(final),
        out_specs=[wide, wide, VMEM],
        scratch_shapes=[pltpu.VMEM((sum(t.shape[0] for t in final) + 8,) + row, BF16), pltpu.VMEM((tile,) + row, BF16), pltpu.SemaphoreType.DMA((len(final),))],
        compiler_params=params(), name='combine',
    )(fpos, x_in, gate, grad_y, *final)
    return y_out, grad_x, grad_gate.reshape(n_tokens, 1), grads[0], grads[1]


def solution(mesh):
    groups = mesh.shape['expert']
    tok_spec = P(('data', 'expert'), None)
    weight_spec = P('expert', None, None)
    grad_spec = P(('data', 'expert'), None, None)

    def device_pass(x_in, expert_idx, gate_weight, grad_y, w_in, w_out):
        sds = jax.ShapeDtypeStruct
        n_tokens, d_model = x_in.shape
        local_experts = w_in.shape[0]
        capacity = (CAP_NUM * n_tokens) // (CAP_DEN * local_experts)
        token_rows = n_tokens // LANES
        sibling = [(i, i ^ 1) for i in range(groups)]
        idx = expert_idx.reshape(token_rows, LANES)
        gate = gate_weight.reshape(token_rows, LANES)
        core = lax.rem(lax.axis_index('expert'), CORES)
        other = lax.ppermute(idx, 'expert', sibling)
        idx2 = jnp.where(core == 0, jnp.concatenate([idx, other]), jnp.concatenate([other, idx]))
        tile = 256
        wide = pl.BlockSpec((tile, d_model), lambda i: (i, 0))
        own_rows = pl.pallas_call(
            functools.partial(build_kernel, tile),
            grid=(n_tokens // tile,),
            out_shape=sds((n_tokens, 2, d_model), BF16),
            in_specs=[wide, VMEM, wide],
            out_specs=pl.BlockSpec((tile, 2, d_model), lambda i: (i, 0, 0)),
            compiler_params=params(), name='build',
        )(x_in, gate, grad_y)
        rank, every = pl.pallas_call(
            functools.partial(count_kernel, groups),
            out_shape=[sds((CORES * token_rows, LANES), I32), sds((groups, LANES), I32)],
            in_specs=[VMEM], out_specs=[VMEM] * 2,
            scratch_shapes=[pltpu.VMEM((8, LANES), I32), pltpu.VMEM((groups, 8, LANES), I32),
                            pltpu.SemaphoreType.DMA((groups,)), pltpu.SemaphoreType.DMA((groups,))],
            cost_estimate=pl.CostEstimate(flops=20 * 10 ** 6, bytes_accessed=10 ** 6, transcendentals=0),
            compiler_params=pltpu.CompilerParams(collective_id=0, has_side_effects=True), name='count',
        )(idx2)
        need = pl.pallas_call(
            functools.partial(need_kernel, capacity, local_experts),
            out_shape=sds((1, LANES), I32), in_specs=[VMEM], out_specs=VMEM, name='need',
        )(every)[0, 0]

        def by_lists(half):
            def run(x, g, i, *rest):
                return list_pass(groups, half, x, g, *rest)

            return run

        branches = [by_lists(half) for half in HALVES]
        branches.append(lambda x, g, i, dy, wi, wo, *rest: padded_pass(groups, x, i, g.reshape(n_tokens, 1), dy, wi, wo))
        which = sum((need > 2 * half).astype(I32) for half in HALVES)
        return lax.switch(which, branches, x_in, gate, expert_idx, grad_y, w_in, w_out, idx2, rank, every, own_rows)

    return jax.shard_map(device_pass, mesh=mesh,
                         in_specs=(tok_spec, tok_spec, tok_spec, tok_spec, weight_spec, weight_spec),
                         out_specs=(tok_spec, tok_spec, tok_spec, grad_spec, grad_spec), check_vma=False)
```

```python
import functools

import jax
import jax.numpy as jnp
from jax import lax
from jax.experimental import pallas as pl
from jax.experimental.pallas import tpu as pltpu
from jax.sharding import PartitionSpec as P


CAP_NUM = 5
CAP_DEN = 4
PAIR_FACTOR = 2
PARTS = (4, 8, 4)
FIRSTS = (0, 4, 12)
CHUNKS = len(PARTS)
UNITS = (88, 96, 128)
LOCAL = 64
CORES = 2
LANES = 128
BIG = 60 * 2 ** 20
F32 = jnp.float32
BF16 = jnp.bfloat16
I32 = jnp.int32
GELU_C = 0.7978845608028654
GELU_A = 0.044715
VMEM = pl.BlockSpec(memory_space=pltpu.VMEM)
SMEM = pl.BlockSpec(memory_space=pltpu.SMEM)
ANY = pl.BlockSpec(memory_space=pl.ANY)


def local_ranks(flat_idx, num_experts):
    one_hot = (flat_idx[:, None] == jnp.arange(num_experts, dtype=jnp.int32)[None, :]).astype(jnp.int32)
    running = jnp.cumsum(one_hot, axis=0)
    return jnp.sum((running - one_hot) * one_hot, axis=1), running[-1]


def exchange_maps(flat_idx, local_rank, counts_all, my_index, local_experts, capacity, pair_cap):
    groups, num_experts = counts_all.shape
    n_pairs = flat_idx.shape[0]
    through = jnp.cumsum(counts_all, axis=0)
    before = through - counts_all
    kept_all = jnp.clip(capacity - before, 0, counts_all)
    before_mine = lax.dynamic_index_in_dim(before, my_index, 0, keepdims=False)
    kept_grid = lax.dynamic_index_in_dim(kept_all, my_index, 0, keepdims=False).reshape(groups, local_experts)
    send_start = (jnp.cumsum(kept_grid, axis=1) - kept_grid).reshape(num_experts)
    pair_slot = before_mine[flat_idx] + local_rank
    target = jnp.where(pair_slot < capacity, (flat_idx // local_experts) * pair_cap + send_start[flat_idx] + local_rank, groups * pair_cap)
    send_src = jnp.full((groups * pair_cap,), n_pairs, jnp.int32).at[target].set(jnp.arange(n_pairs, dtype=jnp.int32), mode='drop')
    first_expert = my_index * local_experts
    through_own = lax.dynamic_slice_in_dim(through, first_expert, local_experts, axis=1)
    before_own = lax.dynamic_slice_in_dim(before, first_expert, local_experts, axis=1)
    kept_own = lax.dynamic_slice_in_dim(kept_all, first_expert, local_experts, axis=1)
    start_own = jnp.cumsum(kept_own, axis=1) - kept_own
    slot_ids = jnp.arange(capacity, dtype=jnp.int32)
    source_dev = jnp.sum((through_own.T[:, None, :] <= slot_ids[None, :, None]).astype(jnp.int32), axis=2)
    filled = slot_ids[None, :] < jnp.minimum(through_own[-1], capacity)[:, None]
    source_dev = jnp.minimum(source_dev, groups - 1)
    start_at = jnp.take_along_axis(start_own.T, source_dev, axis=1)
    before_at = jnp.take_along_axis(before_own.T, source_dev, axis=1)
    recv_pos = jnp.where(filled, source_dev * pair_cap + start_at + slot_ids[None, :] - before_at, groups * pair_cap).reshape(local_experts * capacity)
    back_src = jnp.full((groups * pair_cap,), local_experts * capacity, jnp.int32).at[recv_pos].set(jnp.arange(local_experts * capacity, dtype=jnp.int32), mode='drop')
    return target, send_src, recv_pos, back_src


def exchange(rows):
    return lax.all_to_all(rows, 'expert', 0, 0, tiled=True)


def gather_rows(table, positions):
    return jnp.take(table, positions, axis=0, mode='fill', fill_value=0)


def padded_pass(groups, x_in, expert_idx, gate_weight, grad_y, w_in, w_out):
    n_tokens, top_k = expert_idx.shape
    local_experts, d_model = w_in.shape[0], w_in.shape[1]
    num_experts = local_experts * groups
    n_pairs = n_tokens * top_k
    capacity = (CAP_NUM * n_pairs * groups) // (CAP_DEN * num_experts)
    pair_cap = PAIR_FACTOR * n_pairs // groups
    my_index = lax.axis_index('expert')
    flat_idx = expert_idx.reshape(n_pairs)
    local_rank, counts = local_ranks(flat_idx, num_experts)
    counts_all = lax.all_gather(counts, 'expert')
    target, send_src, recv_pos, back_src = exchange_maps(flat_idx, local_rank, counts_all, my_index, local_experts, capacity, pair_cap)
    exp_rows = gather_rows(exchange(gather_rows(x_in, send_src // top_k)), recv_pos).reshape(local_experts, capacity, d_model)
    pre_act = jnp.einsum('lcd,ldf->lcf', exp_rows, w_in, preferred_element_type=jnp.float32)
    act_full, gelu_pull = jax.vjp(jax.nn.gelu, pre_act)
    act_bf = act_full.astype(jnp.bfloat16)
    out_rows = jnp.einsum('lcf,lfd->lcd', act_bf, w_out, preferred_element_type=jnp.float32).astype(jnp.bfloat16)
    back_out = gather_rows(out_rows.reshape(local_experts * capacity, d_model), back_src)
    out_pair = gather_rows(exchange(back_out), target).reshape(n_tokens, top_k, d_model)
    y_out = (x_in.astype(jnp.float32) + jnp.sum(gate_weight[:, :, None] * out_pair, axis=1)).astype(jnp.bfloat16)
    grad_gate = jnp.einsum('tkd,td->tk', out_pair, grad_y, preferred_element_type=jnp.float32)
    scaled_grad = (gate_weight[:, :, None] * grad_y[:, None, :]).astype(jnp.bfloat16).reshape(n_pairs, d_model)
    grad_rows = gather_rows(exchange(gather_rows(scaled_grad, send_src)), recv_pos).reshape(local_experts, capacity, d_model)
    grad_act = jnp.einsum('lcd,lfd->lcf', grad_rows, w_out, preferred_element_type=jnp.float32).astype(jnp.bfloat16)
    grad_pre = gelu_pull(grad_act.astype(jnp.float32))[0].astype(jnp.bfloat16)
    grad_w_out = jnp.einsum('lcf,lcd->lfd', act_bf, grad_rows, preferred_element_type=jnp.float32).astype(jnp.bfloat16)
    grad_w_in = jnp.einsum('lcd,lcf->ldf', exp_rows, grad_pre, preferred_element_type=jnp.float32).astype(jnp.bfloat16)
    grad_in_rows = jnp.einsum('lcf,ldf->lcd', grad_pre, w_in, preferred_element_type=jnp.float32).astype(jnp.bfloat16)
    back_grad = gather_rows(grad_in_rows.reshape(local_experts * capacity, d_model), back_src)
    grad_pair = gather_rows(exchange(back_grad), target).reshape(n_tokens, top_k, d_model)
    grad_x = (grad_y.astype(jnp.float32) + jnp.sum(grad_pair, axis=1, dtype=jnp.float32)).astype(jnp.bfloat16)
    return y_out, grad_x, grad_gate, grad_w_in, grad_w_out


def iota(shape, dim):
    return lax.broadcasted_iota(jnp.int32, shape, dim)


def exact_dot(a, b):
    return jnp.dot(a, b, preferred_element_type=F32, precision=lax.Precision.HIGHEST)


def xor_chip(a, b):
    return lax.rem(lax.div(a, 2) + lax.div(b, 2), 2) * 2 + lax.rem(lax.rem(a, 2) + lax.rem(b, 2), 2)


def chunk_of(el):
    return sum((el >= first).astype(I32) for first in FIRSTS[1:])


def by_chunk(group, values):
    out = jnp.full(group.shape, values[0], I32)
    for c in range(1, CHUNKS):
        out = jnp.where(group == c, values[c], out)
    return out


def sizes(unit, capacity, chips):
    slot_rows = (capacity + LANES - 1) // LANES
    halves = [unit * p for p in PARTS]
    regions = [(chips - 1) * h + (unit + LOCAL) * p for h, p in zip(halves, PARTS)]
    finals = [2 * (chips - 1) * h + CORES * p * capacity for h, p in zip(halves, PARTS)]
    return slot_rows, halves, [sum(regions[:c]) for c in range(CHUNKS + 1)], [sum(finals[:c]) for c in range(CHUNKS + 1)]


def sum_rows(m):
    return jnp.sum(m, axis=0, keepdims=True)


def count_kernel(groups, idx_ref, rank_ref, every_ref, mine, every, send_sem, recv_sem):
    me = lax.axis_index('expert')
    core = lax.rem(me, CORES)
    rows = idx_ref.shape[0] // CORES
    barrier = pltpu.get_barrier_semaphore()
    for s in range(1, groups):
        pl.semaphore_signal(barrier, inc=1, device_id={'expert': lax.rem(me + s, groups)}, device_id_type=pl.DeviceIdType.MESH)

    def one_hot(r):
        return jnp.where(iota((LANES, LANES), 0) == idx_ref[pl.ds(r, 1), :], 1.0, 0.0)

    seen = jnp.zeros((LANES, LANES), F32)
    for r in range(rows):
        seen = seen + one_hot(core * rows + r)
    counts = lax.dot_general(jnp.ones((8, LANES), BF16), seen.astype(BF16), (((1,), (1,)), ((), ())), preferred_element_type=F32)
    mine[...] = counts.astype(I32)
    every[pl.ds(me, 1)] = counts.astype(I32)[None]
    pl.semaphore_wait(barrier, groups - 1)
    copies = []
    for s in range(1, groups):
        copy = pltpu.make_async_remote_copy(src_ref=mine, dst_ref=every.at[me], send_sem=send_sem.at[s], recv_sem=recv_sem.at[s],
                                            device_id={'expert': lax.rem(me + s, groups)}, device_id_type=pl.DeviceIdType.MESH)
        copy.start()
        copies.append(copy)
    earlier = jnp.where(iota((LANES, LANES), 0) < iota((LANES, LANES), 1), 1.0, 0.0)
    mix = jnp.concatenate([earlier, jnp.ones((LANES, LANES), F32)], axis=0).astype(BF16)
    done = jnp.zeros((LANES, LANES), F32)
    for r in range(rows * CORES):
        hot = one_hot(r)
        rank = jnp.dot(jnp.concatenate([hot, done], axis=1).astype(BF16), mix, preferred_element_type=F32)
        rank_ref[r:r + 1, :] = sum_rows(hot * rank).astype(I32)
        done = done + hot
    for copy in copies:
        copy.wait()
    every_ref[...] = every[:, 0, :]


def chip_tables(cnt, capacity, local_experts):
    groups = cnt.shape[0]
    source = iota((groups, LANES), 0)
    before = jnp.zeros((groups, LANES), F32)
    for i in range(groups - 1):
        before = before + jnp.where(source > i, cnt[i:i + 1, :], 0.0)
    kept = jnp.clip(capacity - before, 0.0, cnt)
    chips = groups // CORES
    k2 = jnp.concatenate([kept[CORES * c:CORES * c + 1] + kept[CORES * c + 1:CORES * c + 2] for c in range(chips)], axis=0)
    b0 = jnp.concatenate([before[CORES * c:CORES * c + 1] for c in range(chips)], axis=0)
    e0, e1 = iota((LANES, LANES), 0), iota((LANES, LANES), 1)
    chip_experts = CORES * local_experts
    same = (lax.div(e0, chip_experts) == lax.div(e1, chip_experts)) & (chunk_of(lax.rem(e0, local_experts)) == chunk_of(lax.rem(e1, local_experts)))
    k8 = jnp.concatenate([k2, k2], axis=0)
    start = exact_dot(k8, jnp.where(same & (e0 < e1), 1.0, 0.0))[:chips]
    same = same & (lax.div(e0, local_experts) == lax.div(e1, local_experts))
    local = exact_dot(k8, jnp.where(same & (e0 < e1), 1.0, 0.0))[:chips]
    return k2, b0, start, local


def need_kernel(capacity, local_experts, every_ref, need_ref):
    k2, _, start, local = chip_tables(every_ref[...].astype(F32), capacity, local_experts)
    away = iota(k2.shape, 0) != lax.div(iota(k2.shape, 1), CORES * local_experts)
    part = by_chunk(chunk_of(lax.rem(iota(k2.shape, 1), local_experts)), PARTS).astype(F32)
    asked = jnp.where(away, (start + k2) * (1.0 / CORES), local + k2 - LOCAL * part) * (float(max(PARTS)) / part)
    longest = jnp.max(asked, axis=0, keepdims=True)
    need_ref[...] = jnp.broadcast_to(jnp.ceil(jnp.max(longest, axis=1, keepdims=True)), (1, LANES)).astype(I32)


def map_kernel(capacity, local_experts, unit, idx_ref, rank_ref, every_ref, inv_ref, recv_ref, fpos_ref, fill_ref, *refs):
    ret_refs, (cols, fall) = refs[:CHUNKS], refs[CHUNKS:]
    me = lax.axis_index('expert')
    core, chip = lax.rem(me, CORES), lax.div(me, CORES)
    rows = idx_ref.shape[0] // CORES
    k2, b0, start, local = chip_tables(every_ref[...].astype(F32), capacity, local_experts)
    chips = k2.shape[0]
    mine = iota(k2.shape, 0) == chip
    pad = jnp.zeros((LANES - 4 * chips, LANES), F32)
    cols[...] = jnp.transpose(jnp.concatenate([k2, b0, start, local, pad], axis=0)).astype(I32)
    look = jnp.concatenate([sum_rows(jnp.where(mine, v, 0.0)) for v in (k2, b0, start, local)], axis=0)
    high = jnp.floor(look * (1.0 / LANES))
    look = jnp.concatenate([high, look - LANES * high], axis=0).astype(BF16)
    slot_rows, halves, regions, finals = sizes(unit, capacity, chips)
    n_high = (regions[-1] + 8 * LANES - 1) // (8 * LANES) * 8
    acc = jnp.zeros((2 * n_high, LANES), F32)
    lane = iota((1, LANES), 1)
    nt = (((1,), (1,)), ((), ()))
    for r in range(rows * CORES):
        e = idx_ref[r:r + 1, :]
        hot = jnp.where(iota((LANES, LANES), 0) == e, 1.0, 0.0).astype(BF16)
        found = jnp.dot(look, hot, preferred_element_type=F32).astype(I32)
        found = found[0:4] * LANES + found[4:8]
        rank = rank_ref[r:r + 1, :]
        slot = found[1:2] + rank
        q = found[2:3] + rank
        owner = lax.div(e, local_experts)
        el = lax.rem(e, local_experts)
        group = chunk_of(el)
        el = el - by_chunk(group, FIRSTS)
        part = by_chunk(group, PARTS)
        half = unit * part
        part_rows = part * capacity
        m = xor_chip(lax.div(owner, CORES), chip)
        here = q - core * half
        local_at = (chips - 1) * half + found[3:4] + rank
        pos = by_chunk(group, regions) + jnp.where(m > 0, (m - 1) * half + here, local_at)
        kept = rank < found[0:1]
        in_half = (here >= 0) & (here < half)
        valid = kept & (((m > 0) & in_half) | ((m == 0) & (owner == me)))
        pos = jnp.where(valid, pos, -1)
        hi = jnp.where(iota((n_high, LANES), 0) == jnp.where(valid, lax.div(pos, LANES), -1), 1.0, 0.0)
        lo = jnp.where(iota((LANES, LANES), 0) == lax.rem(pos, LANES), 1.0, 0.0).astype(BF16)
        row_id = (r % rows + jnp.where(core == r // rows, 0, rows)).astype(F32)
        left = jnp.concatenate([hi * row_id, hi * lane.astype(F32)], axis=0).astype(BF16)
        acc = acc + lax.dot_general(left, lo, nt, preferred_element_type=F32)
        other = (chips - 1) * half
        in_list = jnp.where(in_half, 0, other) + (m - 1) * half + jnp.where(in_half, here, q - (1 - core) * half)
        in_own = 2 * other + jnp.where(owner == me, 0, part_rows) + el * capacity + slot
        fall[r:r + 1, :] = jnp.where(kept, by_chunk(group, finals) + jnp.where(m > 0, in_list, in_own), finals[-1])
    fpos_ref[...] = fall[pl.ds(core * rows, rows), :]
    inv = (acc[:n_high] * LANES + acc[n_high:]).astype(I32)
    inv_ref[...] = inv
    for c, (first_el, part, half) in enumerate(zip(FIRSTS, PARTS, halves)):
        lists, part_rows = (chips - 1) * half, part * capacity
        col = cols[pl.ds(me * local_experts + first_el, part), :]
        total = col[:, 0:1]
        for i in range(1, chips):
            total = total + col[:, i:i + 1]
        fill_ref[first_el:first_el + part, :] = jnp.broadcast_to(total, (part, LANES))
        for j in range(slot_rows):
            s = j * LANES + iota((part, LANES), 1)
            at = jnp.zeros((part, LANES), I32)
            for src in range(chips):
                rel = s - col[:, chips + src:chips + src + 1]
                q = col[:, 2 * chips + src:2 * chips + src + 1] + rel
                here = q - core * half
                away = xor_chip(src, chip)
                remote = jnp.where((here >= 0) & (here < half), 0, lists) + (away - 1) * half + jnp.where((here >= 0) & (here < half), here, q - (1 - core) * half)
                own = 2 * lists + col[:, 3 * chips + src:3 * chips + src + 1] + rel
                at = jnp.where((rel >= 0) & (rel < col[:, src:src + 1]), jnp.where(away > 0, remote, own), at)
            row = slot_rows * first_el + j * part
            recv_ref[row:row + part, :] = at
        q = core * half + iota((part, half), 1)
        for m in range(1, chips):
            src = xor_chip(m, chip)
            at = jnp.zeros((1, half), I32)
            for o in range(CORES):
                col = cols[pl.ds((chip * CORES + o) * local_experts + first_el, part), :]

                def pick(base):
                    return jnp.sum(jnp.where(iota((part, LANES), 1) == base + src, col, 0), axis=1, keepdims=True)

                rel = q - pick(2 * chips)
                base = jnp.where(core == o, 0, part_rows) + iota((part, 1), 0) * capacity
                hit = (rel >= 0) & (rel < pick(0))
                at = at + sum_rows(jnp.where(hit, base + rel + pick(chips), 0))
            ret_refs[c][m - 1:m, :] = at


def column(row):
    return jnp.transpose(jnp.broadcast_to(row, (LANES, LANES)))


def join_rows(first, second, out, at, n, stage):
    for j in range(first.shape[1] // LANES):
        span = slice(j * LANES, (j + 1) * LANES)
        stage[j, pl.ds(0, n, 2), :] = first[:, span].astype(F32)
        stage[j, pl.ds(1, n, 2), :] = second[:, span].astype(F32)
        out[pl.ds(at, n), :, span] = stage[j, pl.ds(0, 2 * n), :].reshape(n, 2, LANES).astype(BF16)


def split_rows(rows, at, n, stage):
    halves = [], []
    for j in range(rows.shape[2] // LANES):
        stage[j, pl.ds(0, 2 * n), :] = rows[pl.ds(at, n), :, j * LANES:(j + 1) * LANES].astype(F32).reshape(2 * n, LANES)
        for k in range(2):
            halves[k].append(stage[j, pl.ds(k, n, 2), :])
    return [jnp.concatenate(h, axis=1) for h in halves]


def build_kernel(tile, x_ref, gate_ref, dy_ref, out_ref, *stages):
    step = pl.program_id(0)
    for q in range(tile // LANES):
        block = pl.ds(q * LANES, LANES)
        gate = column(gate_ref[pl.ds(step * (tile // LANES) + q, 1), :])
        gate = jnp.concatenate([gate] * (x_ref.shape[1] // LANES), axis=1)
        join_rows(x_ref[block, :], gate * dy_ref[block, :].astype(F32), out_ref, q * LANES, LANES, stages[q])


def copy_rows(n, unroll, index, table, rows, first=0):
    def body(b, carry):
        for u in range(unroll):
            rows[pl.ds(first + b * unroll + u, 1)] = table[pl.ds(index(b * unroll + u), 1)]
        return carry

    lax.fori_loop(0, n // unroll, body, 0)


def load_tables(pieces, table, sems):
    at = 0
    copies = []
    for i, piece in enumerate(pieces):
        copy = pltpu.make_async_copy(piece, table.at[pl.ds(at, piece.shape[0])], sems.at[i])
        copy.start()
        copies.append(copy)
        at += piece.shape[0]
    for copy in copies:
        copy.wait()


def pick_kernel(n_tables, places, pos_ref, *refs):
    pieces, outs, (table, sems) = refs[:n_tables], refs[n_tables:-2], refs[-2:]
    load_tables(pieces, table, sems)
    for at, out in zip(places, outs):
        copy_rows(out.shape[0], 16, lambda t, at=at: pos_ref[at + t], table, out)


def expert_kernel(n_tables, n_extra, first, part, capacity, f_tile, fill_ref, pos_ref, w_in_ref, w_out_ref, *refs):
    pieces = refs[:n_tables]
    out_ref, gw_in_ref, gw_out_ref, table, rows, stage, sems = refs[n_tables + n_extra:]
    j = pl.program_id(0)

    @pl.when(j == 0)
    def _():
        load_tables(pieces, table, sems)

    for s in range(0, capacity, LANES):
        n = min(LANES, capacity - s)
        base = (((capacity + LANES - 1) // LANES) * first + (s // LANES) * part + j) * LANES
        copy_rows(n, 16, lambda t, base=base: pos_ref[base + t], table, rows, s)
    n = fill_ref[(first + j) * LANES]
    live = iota((capacity, 1), 0) < n
    xb, gb = [jnp.where(live, v, 0.0).astype(BF16) for v in split_rows(rows, 0, capacity, stage)]
    nt = (((1,), (1,)), ((), ()))
    tn = (((0,), (0,)), ((), ()))
    out = back = None
    for f in range(0, w_in_ref.shape[2], f_tile):
        span = slice(f, f + f_tile)
        a = jnp.dot(xb, w_in_ref[0, :, span], preferred_element_type=F32)
        dh = lax.dot_general(gb, w_out_ref[0, span, :], nt, preferred_element_type=F32).astype(BF16).astype(F32)
        a2 = a * a
        th = jnp.tanh(a * (GELU_C + (GELU_C * GELU_A) * a2))
        cdf = 0.5 + 0.5 * th
        h = (a * cdf).astype(BF16)
        slope = cdf + (0.5 * a) * (1.0 - th * th) * (GELU_C + (3.0 * GELU_C * GELU_A) * a2)
        da = (dh * slope).astype(BF16)
        o = jnp.dot(h, w_out_ref[0, span, :], preferred_element_type=F32)
        d = lax.dot_general(da, w_in_ref[0, :, span], nt, preferred_element_type=F32)
        out = o if out is None else out + o
        back = d if back is None else back + d
        gw_out_ref[0, span, :] = lax.dot_general(h, gb, tn, preferred_element_type=F32).astype(BF16)
        gw_in_ref[0, :, span] = lax.dot_general(xb, da, tn, preferred_element_type=F32).astype(BF16)
    join_rows(out, back, out_ref, 0, capacity, stage)


def combine_kernel(tile, n_tables, pos_ref, x_ref, gate_ref, dy_ref, *refs):
    pieces = refs[:n_tables]
    y_ref, dx_ref, dgate_ref, table, rows, stage, sems = refs[n_tables:]
    step = pl.program_id(0)

    @pl.when(step == 0)
    def _():
        table[pl.ds(table.shape[0] - 8, 8)] = jnp.zeros((8,) + table.shape[1:], BF16)
        load_tables(pieces, table, sems)

    copy_rows(tile, 16, lambda t: pos_ref[step * tile + t], table, rows)
    width = x_ref.shape[1]
    for q in range(tile // LANES):
        block = pl.ds(q * LANES, LANES)
        at = pl.ds(step * (tile // LANES) + q, 1)
        gate = column(gate_ref[at, :])
        gate = jnp.concatenate([gate] * (width // LANES), axis=1)
        o, d = split_rows(rows, q * LANES, LANES, stage.at[q])
        dy = dy_ref[block, :].astype(F32)
        y_ref[block, :] = (x_ref[block, :].astype(F32) + gate * o).astype(BF16)
        dx_ref[block, :] = (dy + d).astype(BF16)
        prod = dy * o
        part = prod[:, 0:LANES]
        for k in range(LANES, width, LANES):
            part = part + prod[:, k:k + LANES]
        dgate_ref[at, :] = jnp.sum(jnp.transpose(part), axis=0, keepdims=True)


def params():
    return pltpu.CompilerParams(vmem_limit_bytes=BIG)


def list_pass(groups, unit, x_in, gate, grad_y, w_in, w_out, idx2, rank, every, own_rows):
    sds = jax.ShapeDtypeStruct
    n_tokens, d_model = x_in.shape
    local_experts, _, d_ff = w_in.shape
    chips = groups // CORES
    capacity = (CAP_NUM * n_tokens) // (CAP_DEN * local_experts)
    slot_rows, halves, regions, _ = sizes(unit, capacity, chips)
    n_high = (regions[-1] + 8 * LANES - 1) // (8 * LANES) * 8
    token_rows = n_tokens // LANES
    row = (2, d_model)

    def to_chip(v, m):
        return lax.ppermute(v, 'expert', [(i, i ^ (CORES * m)) for i in range(groups)])

    def to_sibling(v):
        return lax.ppermute(v, 'expert', [(i, i ^ 1) for i in range(groups)])

    sib_rows = to_sibling(own_rows)
    inv, recv, fpos, fill, *ret = pl.pallas_call(
        functools.partial(map_kernel, capacity, local_experts, unit),
        out_shape=[sds((n_high, LANES), I32), sds((slot_rows * local_experts, LANES), I32),
                   sds((token_rows, LANES), I32), sds((local_experts, LANES), I32)] + [sds((chips - 1, half), I32) for half in halves],
        in_specs=[VMEM] * 3, out_specs=[VMEM] * (4 + CHUNKS),
        scratch_shapes=[pltpu.VMEM((LANES, LANES), I32), pltpu.VMEM((CORES * token_rows, LANES), I32)],
        compiler_params=params(), name='maps',
        cost_estimate=pl.CostEstimate(flops=40 * 10 ** 6, bytes_accessed=10 ** 6, transcendentals=0),
    )(idx2, rank, every)
    inv, recv, fpos, fill, *ret = [v.reshape(-1) for v in (inv, recv, fpos, fill, *ret)]

    def pick(tables, index, places):
        n = sum(t.shape[0] for t in tables)
        return pl.pallas_call(
            functools.partial(pick_kernel, len(tables), [at for at, _ in places]),
            out_shape=[sds((size,) + row, BF16) for _, size in places],
            in_specs=[SMEM] + [ANY] * len(tables), out_specs=[VMEM] * len(places),
            scratch_shapes=[pltpu.VMEM((n,) + row, BF16), pltpu.SemaphoreType.DMA((len(tables),))],
            cost_estimate=pl.CostEstimate(flops=20 * 10 ** 6, bytes_accessed=2 * n * 4 * d_model, transcendentals=0),
            compiler_params=params(),
        )(index, *tables)

    places = [[(regions[c] + m * halves[c], halves[c]) for m in range(chips - 1)] for c in range(CHUNKS)]
    picked = pick([own_rows, sib_rows], inv, places[0])
    here = [(regions[c] + (chips - 1) * halves[c], (unit + LOCAL) * PARTS[c]) for c in range(CHUNKS)]
    picked += pick([own_rows, sib_rows], inv, sum(places[1:], []) + here)
    local = picked[-CHUNKS:]
    arrived = []
    for c in range(CHUNKS):
        got = [to_chip(picked[c * (chips - 1) + m], m + 1) for m in range(chips - 1)]
        arrived.append(got + [to_sibling(v) for v in got])
    grads = []
    final = []
    for c, (first, part, half) in enumerate(zip(FIRSTS, PARTS, halves)):
        weight_in = pl.BlockSpec((1, d_model, d_ff), lambda i, first=first: (first + i, 0, 0))
        weight_out = pl.BlockSpec((1, d_ff, d_model), lambda i, first=first: (first + i, 0, 0))
        row_block = pl.BlockSpec((capacity,) + row, lambda i: (i, 0, 0))
        tables = arrived[c] + [local[c]]
        n = len(tables)
        experts = pl.pallas_call(
            functools.partial(expert_kernel, n, len(grads), first, part, capacity, 512),
            grid=(part,),
            out_shape=[sds((part * capacity,) + row, BF16), sds(w_in.shape, BF16), sds(w_out.shape, BF16)],
            in_specs=[SMEM, SMEM, weight_in, weight_out] + [ANY] * (n + len(grads)),
            out_specs=[row_block, weight_in, weight_out],
            input_output_aliases={4 + n: 1, 5 + n: 2} if grads else {},
            scratch_shapes=[pltpu.VMEM((sum(t.shape[0] for t in tables),) + row, BF16), pltpu.VMEM((capacity,) + row, BF16), pltpu.VMEM((d_model // LANES, 2 * capacity, LANES), F32), pltpu.SemaphoreType.DMA((n,))],
            compiler_params=params(),
            cost_estimate=pl.CostEstimate(flops=12 * part * capacity * d_model * d_ff, bytes_accessed=8 * part * d_model * d_ff, transcendentals=part * capacity * d_ff),
            name='experts',
        )
        out_rows, *grads = experts(fill, recv, w_in, w_out, *tables, *grads)
        sib_out = to_sibling(out_rows)
        sent = pick([out_rows, sib_out], ret[c], [(m * half, half) for m in range(chips - 1)])
        got = [to_chip(v, m + 1) for m, v in enumerate(sent)]
        final += got + [to_sibling(v) for v in got] + [out_rows, sib_out]
    tile = 512
    wide = pl.BlockSpec((tile, d_model), lambda i: (i, 0))
    y_out, grad_x, grad_gate = pl.pallas_call(
        functools.partial(combine_kernel, tile, len(final)),
        grid=(n_tokens // tile,),
        out_shape=[sds(x_in.shape, BF16), sds(x_in.shape, BF16), sds((token_rows, LANES), F32)],
        in_specs=[SMEM, wide, VMEM, wide] + [ANY] * len(final),
        out_specs=[wide, wide, VMEM],
        scratch_shapes=[pltpu.VMEM((sum(t.shape[0] for t in final) + 8,) + row, BF16), pltpu.VMEM((tile,) + row, BF16), pltpu.VMEM((tile // LANES, d_model // LANES, 2 * LANES, LANES), F32), pltpu.SemaphoreType.DMA((len(final),))],
        compiler_params=params(), name='combine',
    )(fpos, x_in, gate, grad_y, *final)
    return y_out, grad_x, grad_gate.reshape(n_tokens, 1), grads[0], grads[1]


def solution(mesh):
    groups = mesh.shape['expert']
    tok_spec = P(('data', 'expert'), None)
    weight_spec = P('expert', None, None)
    grad_spec = P(('data', 'expert'), None, None)

    def device_pass(x_in, expert_idx, gate_weight, grad_y, w_in, w_out):
        sds = jax.ShapeDtypeStruct
        n_tokens, d_model = x_in.shape
        local_experts = w_in.shape[0]
        capacity = (CAP_NUM * n_tokens) // (CAP_DEN * local_experts)
        token_rows = n_tokens // LANES
        sibling = [(i, i ^ 1) for i in range(groups)]
        idx = expert_idx.reshape(token_rows, LANES)
        gate = gate_weight.reshape(token_rows, LANES)
        core = lax.rem(lax.axis_index('expert'), CORES)
        other = lax.ppermute(idx, 'expert', sibling)
        idx2 = jnp.where(core == 0, jnp.concatenate([idx, other]), jnp.concatenate([other, idx]))
        tile = 512
        wide = pl.BlockSpec((tile, d_model), lambda i: (i, 0))
        own_rows = pl.pallas_call(
            functools.partial(build_kernel, tile),
            grid=(n_tokens // tile,),
            out_shape=sds((n_tokens, 2, d_model), BF16),
            in_specs=[wide, VMEM, wide],
            out_specs=pl.BlockSpec((tile, 2, d_model), lambda i: (i, 0, 0)),
            scratch_shapes=[pltpu.VMEM((d_model // LANES, 2 * LANES, LANES), F32)] * (tile // LANES),
            compiler_params=params(), name='build',
        )(x_in, gate, grad_y)
        rank, every = pl.pallas_call(
            functools.partial(count_kernel, groups),
            out_shape=[sds((CORES * token_rows, LANES), I32), sds((groups, LANES), I32)],
            in_specs=[VMEM], out_specs=[VMEM] * 2,
            scratch_shapes=[pltpu.VMEM((8, LANES), I32), pltpu.VMEM((groups, 8, LANES), I32),
                            pltpu.SemaphoreType.DMA((groups,)), pltpu.SemaphoreType.DMA((groups,))],
            cost_estimate=pl.CostEstimate(flops=20 * 10 ** 6, bytes_accessed=10 ** 6, transcendentals=0),
            compiler_params=pltpu.CompilerParams(collective_id=0, has_side_effects=True), name='count',
        )(idx2)
        need = pl.pallas_call(
            functools.partial(need_kernel, capacity, local_experts),
            out_shape=sds((1, LANES), I32), in_specs=[VMEM], out_specs=VMEM, name='need',
        )(every)[0, 0]

        def by_lists(half):
            def run(x, g, i, *rest):
                return list_pass(groups, half, x, g, *rest)

            return run

        branches = [by_lists(half) for half in UNITS]
        branches.append(lambda x, g, i, dy, wi, wo, *rest: padded_pass(groups, x, i, g.reshape(n_tokens, 1), dy, wi, wo))
        operands = (x_in, gate, expert_idx, grad_y, w_in, w_out, idx2, rank, every, own_rows)

        def choose(n):
            if n == len(UNITS):
                return branches[n]
            return lambda *a: lax.cond(need <= max(PARTS) * UNITS[n], branches[n], choose(n + 1), *a)

        return choose(0)(*operands)

    return jax.shard_map(device_pass, mesh=mesh,
                         in_specs=(tok_spec, tok_spec, tok_spec, tok_spec, weight_spec, weight_spec),
                         out_specs=(tok_spec, tok_spec, tok_spec, grad_spec, grad_spec), check_vma=False)
```

```python
import functools

import jax
import jax.numpy as jnp
from jax import lax
from jax.experimental import pallas as pl
from jax.experimental.pallas import tpu as pltpu
from jax.sharding import PartitionSpec as P


CAP_NUM = 5
CAP_DEN = 4
PAIR_FACTOR = 2
PARTS = (4, 8, 4)
FIRSTS = (0, 4, 12)
CHUNKS = len(PARTS)
UNITS = (96, 128)
LOCAL = 64
CORES = 2
LANES = 128
BIG = 60 * 2 ** 20
F32 = jnp.float32
BF16 = jnp.bfloat16
I32 = jnp.int32
GELU_C = 0.7978845608028654
GELU_A = 0.044715
VMEM = pl.BlockSpec(memory_space=pltpu.VMEM)
SMEM = pl.BlockSpec(memory_space=pltpu.SMEM)
ANY = pl.BlockSpec(memory_space=pl.ANY)


def local_ranks(flat_idx, num_experts):
    one_hot = (flat_idx[:, None] == jnp.arange(num_experts, dtype=jnp.int32)[None, :]).astype(jnp.int32)
    running = jnp.cumsum(one_hot, axis=0)
    return jnp.sum((running - one_hot) * one_hot, axis=1), running[-1]


def exchange_maps(flat_idx, local_rank, counts_all, my_index, local_experts, capacity, pair_cap):
    groups, num_experts = counts_all.shape
    n_pairs = flat_idx.shape[0]
    through = jnp.cumsum(counts_all, axis=0)
    before = through - counts_all
    kept_all = jnp.clip(capacity - before, 0, counts_all)
    before_mine = lax.dynamic_index_in_dim(before, my_index, 0, keepdims=False)
    kept_grid = lax.dynamic_index_in_dim(kept_all, my_index, 0, keepdims=False).reshape(groups, local_experts)
    send_start = (jnp.cumsum(kept_grid, axis=1) - kept_grid).reshape(num_experts)
    pair_slot = before_mine[flat_idx] + local_rank
    target = jnp.where(pair_slot < capacity, (flat_idx // local_experts) * pair_cap + send_start[flat_idx] + local_rank, groups * pair_cap)
    send_src = jnp.full((groups * pair_cap,), n_pairs, jnp.int32).at[target].set(jnp.arange(n_pairs, dtype=jnp.int32), mode='drop')
    first_expert = my_index * local_experts
    through_own = lax.dynamic_slice_in_dim(through, first_expert, local_experts, axis=1)
    before_own = lax.dynamic_slice_in_dim(before, first_expert, local_experts, axis=1)
    kept_own = lax.dynamic_slice_in_dim(kept_all, first_expert, local_experts, axis=1)
    start_own = jnp.cumsum(kept_own, axis=1) - kept_own
    slot_ids = jnp.arange(capacity, dtype=jnp.int32)
    source_dev = jnp.sum((through_own.T[:, None, :] <= slot_ids[None, :, None]).astype(jnp.int32), axis=2)
    filled = slot_ids[None, :] < jnp.minimum(through_own[-1], capacity)[:, None]
    source_dev = jnp.minimum(source_dev, groups - 1)
    start_at = jnp.take_along_axis(start_own.T, source_dev, axis=1)
    before_at = jnp.take_along_axis(before_own.T, source_dev, axis=1)
    recv_pos = jnp.where(filled, source_dev * pair_cap + start_at + slot_ids[None, :] - before_at, groups * pair_cap).reshape(local_experts * capacity)
    back_src = jnp.full((groups * pair_cap,), local_experts * capacity, jnp.int32).at[recv_pos].set(jnp.arange(local_experts * capacity, dtype=jnp.int32), mode='drop')
    return target, send_src, recv_pos, back_src


def exchange(rows):
    return lax.all_to_all(rows, 'expert', 0, 0, tiled=True)


def gather_rows(table, positions):
    return jnp.take(table, positions, axis=0, mode='fill', fill_value=0)


def padded_pass(groups, x_in, expert_idx, gate_weight, grad_y, w_in, w_out):
    n_tokens, top_k = expert_idx.shape
    local_experts, d_model = w_in.shape[0], w_in.shape[1]
    num_experts = local_experts * groups
    n_pairs = n_tokens * top_k
    capacity = (CAP_NUM * n_pairs * groups) // (CAP_DEN * num_experts)
    pair_cap = PAIR_FACTOR * n_pairs // groups
    my_index = lax.axis_index('expert')
    flat_idx = expert_idx.reshape(n_pairs)
    local_rank, counts = local_ranks(flat_idx, num_experts)
    counts_all = lax.all_gather(counts, 'expert')
    target, send_src, recv_pos, back_src = exchange_maps(flat_idx, local_rank, counts_all, my_index, local_experts, capacity, pair_cap)
    exp_rows = gather_rows(exchange(gather_rows(x_in, send_src // top_k)), recv_pos).reshape(local_experts, capacity, d_model)
    pre_act = jnp.einsum('lcd,ldf->lcf', exp_rows, w_in, preferred_element_type=jnp.float32)
    act_full, gelu_pull = jax.vjp(jax.nn.gelu, pre_act)
    act_bf = act_full.astype(jnp.bfloat16)
    out_rows = jnp.einsum('lcf,lfd->lcd', act_bf, w_out, preferred_element_type=jnp.float32).astype(jnp.bfloat16)
    back_out = gather_rows(out_rows.reshape(local_experts * capacity, d_model), back_src)
    out_pair = gather_rows(exchange(back_out), target).reshape(n_tokens, top_k, d_model)
    y_out = (x_in.astype(jnp.float32) + jnp.sum(gate_weight[:, :, None] * out_pair, axis=1)).astype(jnp.bfloat16)
    grad_gate = jnp.einsum('tkd,td->tk', out_pair, grad_y, preferred_element_type=jnp.float32)
    scaled_grad = (gate_weight[:, :, None] * grad_y[:, None, :]).astype(jnp.bfloat16).reshape(n_pairs, d_model)
    grad_rows = gather_rows(exchange(gather_rows(scaled_grad, send_src)), recv_pos).reshape(local_experts, capacity, d_model)
    grad_act = jnp.einsum('lcd,lfd->lcf', grad_rows, w_out, preferred_element_type=jnp.float32).astype(jnp.bfloat16)
    grad_pre = gelu_pull(grad_act.astype(jnp.float32))[0].astype(jnp.bfloat16)
    grad_w_out = jnp.einsum('lcf,lcd->lfd', act_bf, grad_rows, preferred_element_type=jnp.float32).astype(jnp.bfloat16)
    grad_w_in = jnp.einsum('lcd,lcf->ldf', exp_rows, grad_pre, preferred_element_type=jnp.float32).astype(jnp.bfloat16)
    grad_in_rows = jnp.einsum('lcf,ldf->lcd', grad_pre, w_in, preferred_element_type=jnp.float32).astype(jnp.bfloat16)
    back_grad = gather_rows(grad_in_rows.reshape(local_experts * capacity, d_model), back_src)
    grad_pair = gather_rows(exchange(back_grad), target).reshape(n_tokens, top_k, d_model)
    grad_x = (grad_y.astype(jnp.float32) + jnp.sum(grad_pair, axis=1, dtype=jnp.float32)).astype(jnp.bfloat16)
    return y_out, grad_x, grad_gate, grad_w_in, grad_w_out


def iota(shape, dim):
    return lax.broadcasted_iota(jnp.int32, shape, dim)


def exact_dot(a, b):
    return jnp.dot(a, b, preferred_element_type=F32, precision=lax.Precision.HIGHEST)


def xor_chip(a, b):
    return lax.rem(lax.div(a, 2) + lax.div(b, 2), 2) * 2 + lax.rem(lax.rem(a, 2) + lax.rem(b, 2), 2)


def chunk_of(el):
    return sum((el >= first).astype(I32) for first in FIRSTS[1:])


def by_chunk(group, values):
    out = jnp.full(group.shape, values[0], I32)
    for c in range(1, CHUNKS):
        out = jnp.where(group == c, values[c], out)
    return out


def sizes(unit, capacity, chips):
    slot_rows = (capacity + LANES - 1) // LANES
    halves = [unit * p for p in PARTS]
    regions = [(chips - 1) * h + (unit + LOCAL) * p for h, p in zip(halves, PARTS)]
    finals = [2 * (chips - 1) * h + CORES * p * capacity for h, p in zip(halves, PARTS)]
    return slot_rows, halves, [sum(regions[:c]) for c in range(CHUNKS + 1)], [sum(finals[:c]) for c in range(CHUNKS + 1)]


def sum_rows(m):
    return jnp.sum(m, axis=0, keepdims=True)


def count_kernel(groups, idx_ref, rank_ref, every_ref, mine, every, send_sem, recv_sem):
    me = lax.axis_index('expert')
    core = lax.rem(me, CORES)
    rows = idx_ref.shape[0] // CORES
    barrier = pltpu.get_barrier_semaphore()
    for s in range(1, groups):
        pl.semaphore_signal(barrier, inc=1, device_id={'expert': lax.rem(me + s, groups)}, device_id_type=pl.DeviceIdType.MESH)

    def one_hot(r):
        return jnp.where(iota((LANES, LANES), 0) == idx_ref[pl.ds(r, 1), :], 1.0, 0.0)

    seen = jnp.zeros((LANES, LANES), F32)
    for r in range(rows):
        seen = seen + one_hot(core * rows + r)
    counts = lax.dot_general(jnp.ones((8, LANES), BF16), seen.astype(BF16), (((1,), (1,)), ((), ())), preferred_element_type=F32)
    mine[...] = counts.astype(I32)
    every[pl.ds(me, 1)] = counts.astype(I32)[None]
    pl.semaphore_wait(barrier, groups - 1)
    copies = []
    for s in range(1, groups):
        copy = pltpu.make_async_remote_copy(src_ref=mine, dst_ref=every.at[me], send_sem=send_sem.at[s], recv_sem=recv_sem.at[s],
                                            device_id={'expert': lax.rem(me + s, groups)}, device_id_type=pl.DeviceIdType.MESH)
        copy.start()
        copies.append(copy)
    earlier = jnp.where(iota((LANES, LANES), 0) < iota((LANES, LANES), 1), 1.0, 0.0)
    mix = jnp.concatenate([earlier, jnp.ones((LANES, LANES), F32)], axis=0).astype(BF16)
    done = jnp.zeros((LANES, LANES), F32)
    for r in range(rows * CORES):
        hot = one_hot(r)
        rank = jnp.dot(jnp.concatenate([hot, done], axis=1).astype(BF16), mix, preferred_element_type=F32)
        rank_ref[r:r + 1, :] = sum_rows(hot * rank).astype(I32)
        done = done + hot
    for copy in copies:
        copy.wait()
    every_ref[...] = every[:, 0, :]


def chip_tables(cnt, capacity, local_experts):
    groups = cnt.shape[0]
    source = iota((groups, LANES), 0)
    before = jnp.zeros((groups, LANES), F32)
    for i in range(groups - 1):
        before = before + jnp.where(source > i, cnt[i:i + 1, :], 0.0)
    kept = jnp.clip(capacity - before, 0.0, cnt)
    chips = groups // CORES
    k2 = jnp.concatenate([kept[CORES * c:CORES * c + 1] + kept[CORES * c + 1:CORES * c + 2] for c in range(chips)], axis=0)
    b0 = jnp.concatenate([before[CORES * c:CORES * c + 1] for c in range(chips)], axis=0)
    e0, e1 = iota((LANES, LANES), 0), iota((LANES, LANES), 1)
    chip_experts = CORES * local_experts
    same = (lax.div(e0, chip_experts) == lax.div(e1, chip_experts)) & (chunk_of(lax.rem(e0, local_experts)) == chunk_of(lax.rem(e1, local_experts)))
    k8 = jnp.concatenate([k2, k2], axis=0)
    start = exact_dot(k8, jnp.where(same & (e0 < e1), 1.0, 0.0))[:chips]
    same = same & (lax.div(e0, local_experts) == lax.div(e1, local_experts))
    local = exact_dot(k8, jnp.where(same & (e0 < e1), 1.0, 0.0))[:chips]
    return k2, b0, start, local


def need_kernel(capacity, local_experts, every_ref, need_ref):
    k2, _, start, local = chip_tables(every_ref[...].astype(F32), capacity, local_experts)
    away = iota(k2.shape, 0) != lax.div(iota(k2.shape, 1), CORES * local_experts)
    part = by_chunk(chunk_of(lax.rem(iota(k2.shape, 1), local_experts)), PARTS).astype(F32)
    asked = jnp.where(away, (start + k2) * (1.0 / CORES), local + k2 - LOCAL * part) * (float(max(PARTS)) / part)
    longest = jnp.max(asked, axis=0, keepdims=True)
    need_ref[...] = jnp.broadcast_to(jnp.ceil(jnp.max(longest, axis=1, keepdims=True)), (1, LANES)).astype(I32)


def map_kernel(capacity, local_experts, unit, idx_ref, rank_ref, every_ref, inv_ref, recv_ref, fpos_ref, fill_ref, *refs):
    ret_refs, (cols, fall) = refs[:CHUNKS], refs[CHUNKS:]
    me = lax.axis_index('expert')
    core, chip = lax.rem(me, CORES), lax.div(me, CORES)
    rows = idx_ref.shape[0] // CORES
    k2, b0, start, local = chip_tables(every_ref[...].astype(F32), capacity, local_experts)
    chips = k2.shape[0]
    mine = iota(k2.shape, 0) == chip
    pad = jnp.zeros((LANES - 4 * chips, LANES), F32)
    cols[...] = jnp.transpose(jnp.concatenate([k2, b0, start, local, pad], axis=0)).astype(I32)
    look = jnp.concatenate([sum_rows(jnp.where(mine, v, 0.0)) for v in (k2, b0, start, local)], axis=0)
    high = jnp.floor(look * (1.0 / LANES))
    look = jnp.concatenate([high, look - LANES * high], axis=0).astype(BF16)
    slot_rows, halves, regions, finals = sizes(unit, capacity, chips)
    n_high = (regions[-1] + 8 * LANES - 1) // (8 * LANES) * 8
    acc = jnp.zeros((2 * n_high, LANES), F32)
    lane = iota((1, LANES), 1)
    nt = (((1,), (1,)), ((), ()))
    for r in range(rows * CORES):
        e = idx_ref[r:r + 1, :]
        hot = jnp.where(iota((LANES, LANES), 0) == e, 1.0, 0.0).astype(BF16)
        found = jnp.dot(look, hot, preferred_element_type=F32).astype(I32)
        found = found[0:4] * LANES + found[4:8]
        rank = rank_ref[r:r + 1, :]
        slot = found[1:2] + rank
        q = found[2:3] + rank
        owner = lax.div(e, local_experts)
        el = lax.rem(e, local_experts)
        group = chunk_of(el)
        el = el - by_chunk(group, FIRSTS)
        part = by_chunk(group, PARTS)
        half = unit * part
        part_rows = part * capacity
        m = xor_chip(lax.div(owner, CORES), chip)
        here = q - core * half
        local_at = (chips - 1) * half + found[3:4] + rank
        pos = by_chunk(group, regions) + jnp.where(m > 0, (m - 1) * half + here, local_at)
        kept = rank < found[0:1]
        in_half = (here >= 0) & (here < half)
        valid = kept & (((m > 0) & in_half) | ((m == 0) & (owner == me)))
        pos = jnp.where(valid, pos, -1)
        hi = jnp.where(iota((n_high, LANES), 0) == jnp.where(valid, lax.div(pos, LANES), -1), 1.0, 0.0)
        lo = jnp.where(iota((LANES, LANES), 0) == lax.rem(pos, LANES), 1.0, 0.0).astype(BF16)
        row_id = (r % rows + jnp.where(core == r // rows, 0, rows)).astype(F32)
        left = jnp.concatenate([hi * row_id, hi * lane.astype(F32)], axis=0).astype(BF16)
        acc = acc + lax.dot_general(left, lo, nt, preferred_element_type=F32)
        other = (chips - 1) * half
        in_list = jnp.where(in_half, 0, other) + (m - 1) * half + jnp.where(in_half, here, q - (1 - core) * half)
        in_own = 2 * other + jnp.where(owner == me, 0, part_rows) + el * capacity + slot
        fall[r:r + 1, :] = jnp.where(kept, by_chunk(group, finals) + jnp.where(m > 0, in_list, in_own), finals[-1])
    fpos_ref[...] = fall[pl.ds(core * rows, rows), :]
    inv = (acc[:n_high] * LANES + acc[n_high:]).astype(I32)
    inv_ref[...] = inv
    for c, (first_el, part, half) in enumerate(zip(FIRSTS, PARTS, halves)):
        lists, part_rows = (chips - 1) * half, part * capacity
        col = cols[pl.ds(me * local_experts + first_el, part), :]
        total = col[:, 0:1]
        for i in range(1, chips):
            total = total + col[:, i:i + 1]
        fill_ref[first_el:first_el + part, :] = jnp.broadcast_to(total, (part, LANES))
        for j in range(slot_rows):
            s = j * LANES + iota((part, LANES), 1)
            at = jnp.zeros((part, LANES), I32)
            for src in range(chips):
                rel = s - col[:, chips + src:chips + src + 1]
                q = col[:, 2 * chips + src:2 * chips + src + 1] + rel
                here = q - core * half
                away = xor_chip(src, chip)
                remote = jnp.where((here >= 0) & (here < half), 0, lists) + (away - 1) * half + jnp.where((here >= 0) & (here < half), here, q - (1 - core) * half)
                own = 2 * lists + col[:, 3 * chips + src:3 * chips + src + 1] + rel
                at = jnp.where((rel >= 0) & (rel < col[:, src:src + 1]), jnp.where(away > 0, remote, own), at)
            row = slot_rows * first_el + j * part
            recv_ref[row:row + part, :] = at
        q = core * half + iota((part, half), 1)
        for m in range(1, chips):
            src = xor_chip(m, chip)
            at = jnp.zeros((1, half), I32)
            for o in range(CORES):
                col = cols[pl.ds((chip * CORES + o) * local_experts + first_el, part), :]

                def pick(base):
                    return jnp.sum(jnp.where(iota((part, LANES), 1) == base + src, col, 0), axis=1, keepdims=True)

                rel = q - pick(2 * chips)
                base = jnp.where(core == o, 0, part_rows) + iota((part, 1), 0) * capacity
                hit = (rel >= 0) & (rel < pick(0))
                at = at + sum_rows(jnp.where(hit, base + rel + pick(chips), 0))
            ret_refs[c][m - 1:m, :] = at


def column(row):
    return jnp.transpose(jnp.broadcast_to(row, (LANES, LANES)))


def join_rows(first, second, out, at, n, stage):
    for j in range(first.shape[1] // LANES):
        span = slice(j * LANES, (j + 1) * LANES)
        stage[j, pl.ds(0, n, 2), :] = first[:, span].astype(F32)
        stage[j, pl.ds(1, n, 2), :] = second[:, span].astype(F32)
        out[pl.ds(at, n), :, span] = stage[j, pl.ds(0, 2 * n), :].reshape(n, 2, LANES).astype(BF16)


def split_rows(rows, at, n, stage):
    halves = [], []
    for j in range(rows.shape[2] // LANES):
        stage[j, pl.ds(0, 2 * n), :] = rows[pl.ds(at, n), :, j * LANES:(j + 1) * LANES].astype(F32).reshape(2 * n, LANES)
        for k in range(2):
            halves[k].append(stage[j, pl.ds(k, n, 2), :])
    return [jnp.concatenate(h, axis=1) for h in halves]


def build_kernel(tile, x_ref, gate_ref, dy_ref, out_ref, *stages):
    step = pl.program_id(0)
    for q in range(tile // LANES):
        block = pl.ds(q * LANES, LANES)
        gate = column(gate_ref[pl.ds(step * (tile // LANES) + q, 1), :])
        gate = jnp.concatenate([gate] * (x_ref.shape[1] // LANES), axis=1)
        join_rows(x_ref[block, :], gate * dy_ref[block, :].astype(F32), out_ref, q * LANES, LANES, stages[q])


def copy_rows(n, unroll, index, table, rows, first=0):
    def body(b, carry):
        for u in range(unroll):
            rows[pl.ds(first + b * unroll + u, 1)] = table[pl.ds(index(b * unroll + u), 1)]
        return carry

    lax.fori_loop(0, n // unroll, body, 0)


def load_tables(pieces, table, sems):
    at = 0
    copies = []
    for i, piece in enumerate(pieces):
        copy = pltpu.make_async_copy(piece, table.at[pl.ds(at, piece.shape[0])], sems.at[i])
        copy.start()
        copies.append(copy)
        at += piece.shape[0]
    for copy in copies:
        copy.wait()


def pick_kernel(n_tables, places, pos_ref, *refs):
    pieces, outs, (table, sems) = refs[:n_tables], refs[n_tables:-2], refs[-2:]
    load_tables(pieces, table, sems)
    for at, out in zip(places, outs):
        copy_rows(out.shape[0], 16, lambda t, at=at: pos_ref[at + t], table, out)


def expert_kernel(n_tables, n_extra, first, part, capacity, f_tile, fill_ref, pos_ref, w_in_ref, w_out_ref, *refs):
    pieces = refs[:n_tables]
    out_ref, gw_in_ref, gw_out_ref, table, rows, stage, sems = refs[n_tables + n_extra:]
    j = pl.program_id(0)

    @pl.when(j == 0)
    def _():
        load_tables(pieces, table, sems)

    for s in range(0, capacity, LANES):
        n = min(LANES, capacity - s)
        base = (((capacity + LANES - 1) // LANES) * first + (s // LANES) * part + j) * LANES
        copy_rows(n, 16, lambda t, base=base: pos_ref[base + t], table, rows, s)
    n = fill_ref[(first + j) * LANES]
    live = iota((capacity, 1), 0) < n
    xb, gb = [jnp.where(live, v, 0.0).astype(BF16) for v in split_rows(rows, 0, capacity, stage)]
    nt = (((1,), (1,)), ((), ()))
    tn = (((0,), (0,)), ((), ()))
    out = back = None
    for f in range(0, w_in_ref.shape[2], f_tile):
        span = slice(f, f + f_tile)
        a = jnp.dot(xb, w_in_ref[0, :, span], preferred_element_type=F32)
        dh = lax.dot_general(gb, w_out_ref[0, span, :], nt, preferred_element_type=F32).astype(BF16).astype(F32)
        a2 = a * a
        th = jnp.tanh(a * (GELU_C + (GELU_C * GELU_A) * a2))
        cdf = 0.5 + 0.5 * th
        h = (a * cdf).astype(BF16)
        slope = cdf + (0.5 * a) * (1.0 - th * th) * (GELU_C + (3.0 * GELU_C * GELU_A) * a2)
        da = (dh * slope).astype(BF16)
        o = jnp.dot(h, w_out_ref[0, span, :], preferred_element_type=F32)
        d = lax.dot_general(da, w_in_ref[0, :, span], nt, preferred_element_type=F32)
        out = o if out is None else out + o
        back = d if back is None else back + d
        gw_out_ref[0, span, :] = lax.dot_general(h, gb, tn, preferred_element_type=F32).astype(BF16)
        gw_in_ref[0, :, span] = lax.dot_general(xb, da, tn, preferred_element_type=F32).astype(BF16)
    join_rows(out, back, out_ref, 0, capacity, stage)


def combine_kernel(tile, n_tables, pos_ref, x_ref, gate_ref, dy_ref, *refs):
    pieces = refs[:n_tables]
    y_ref, dx_ref, dgate_ref, table, rows, stage, sems = refs[n_tables:]
    step = pl.program_id(0)

    @pl.when(step == 0)
    def _():
        table[pl.ds(table.shape[0] - 8, 8)] = jnp.zeros((8,) + table.shape[1:], BF16)
        load_tables(pieces, table, sems)

    copy_rows(tile, 16, lambda t: pos_ref[step * tile + t], table, rows)
    width = x_ref.shape[1]
    for q in range(tile // LANES):
        block = pl.ds(q * LANES, LANES)
        at = pl.ds(step * (tile // LANES) + q, 1)
        gate = column(gate_ref[at, :])
        gate = jnp.concatenate([gate] * (width // LANES), axis=1)
        o, d = split_rows(rows, q * LANES, LANES, stage.at[q])
        dy = dy_ref[block, :].astype(F32)
        y_ref[block, :] = (x_ref[block, :].astype(F32) + gate * o).astype(BF16)
        dx_ref[block, :] = (dy + d).astype(BF16)
        prod = dy * o
        part = prod[:, 0:LANES]
        for k in range(LANES, width, LANES):
            part = part + prod[:, k:k + LANES]
        dgate_ref[at, :] = jnp.sum(jnp.transpose(part), axis=0, keepdims=True)


def params():
    return pltpu.CompilerParams(vmem_limit_bytes=BIG)


def list_pass(groups, unit, x_in, gate, grad_y, w_in, w_out, idx2, rank, every, own_rows):
    sds = jax.ShapeDtypeStruct
    n_tokens, d_model = x_in.shape
    local_experts, _, d_ff = w_in.shape
    chips = groups // CORES
    capacity = (CAP_NUM * n_tokens) // (CAP_DEN * local_experts)
    slot_rows, halves, regions, _ = sizes(unit, capacity, chips)
    n_high = (regions[-1] + 8 * LANES - 1) // (8 * LANES) * 8
    token_rows = n_tokens // LANES
    row = (2, d_model)

    def to_chip(v, m):
        return lax.ppermute(v, 'expert', [(i, i ^ (CORES * m)) for i in range(groups)])

    def to_sibling(v):
        return lax.ppermute(v, 'expert', [(i, i ^ 1) for i in range(groups)])

    sib_rows = to_sibling(own_rows)
    inv, recv, fpos, fill, *ret = pl.pallas_call(
        functools.partial(map_kernel, capacity, local_experts, unit),
        out_shape=[sds((n_high, LANES), I32), sds((slot_rows * local_experts, LANES), I32),
                   sds((token_rows, LANES), I32), sds((local_experts, LANES), I32)] + [sds((chips - 1, half), I32) for half in halves],
        in_specs=[VMEM] * 3, out_specs=[VMEM] * (4 + CHUNKS),
        scratch_shapes=[pltpu.VMEM((LANES, LANES), I32), pltpu.VMEM((CORES * token_rows, LANES), I32)],
        compiler_params=params(), name='maps',
        cost_estimate=pl.CostEstimate(flops=40 * 10 ** 6, bytes_accessed=10 ** 6, transcendentals=0),
    )(idx2, rank, every)
    inv, recv, fpos, fill, *ret = [v.reshape(-1) for v in (inv, recv, fpos, fill, *ret)]

    def pick(tables, index, places):
        n = sum(t.shape[0] for t in tables)
        return pl.pallas_call(
            functools.partial(pick_kernel, len(tables), [at for at, _ in places]),
            out_shape=[sds((size,) + row, BF16) for _, size in places],
            in_specs=[SMEM] + [ANY] * len(tables), out_specs=[VMEM] * len(places),
            scratch_shapes=[pltpu.VMEM((n,) + row, BF16), pltpu.SemaphoreType.DMA((len(tables),))],
            cost_estimate=pl.CostEstimate(flops=20 * 10 ** 6, bytes_accessed=2 * n * 4 * d_model, transcendentals=0),
            compiler_params=params(),
        )(index, *tables)

    places = [[(regions[c] + m * halves[c], halves[c]) for m in range(chips - 1)] for c in range(CHUNKS)]
    picked = pick([own_rows, sib_rows], inv, places[0])
    here = [(regions[c] + (chips - 1) * halves[c], (unit + LOCAL) * PARTS[c]) for c in range(CHUNKS)]
    picked += pick([own_rows, sib_rows], inv, sum(places[1:], []) + here)
    local = picked[-CHUNKS:]
    arrived = []
    for c in range(CHUNKS):
        got = [to_chip(picked[c * (chips - 1) + m], m + 1) for m in range(chips - 1)]
        arrived.append(got + [to_sibling(v) for v in got])
    grads = []
    final = []
    for c, (first, part, half) in enumerate(zip(FIRSTS, PARTS, halves)):
        weight_in = pl.BlockSpec((1, d_model, d_ff), lambda i, first=first: (first + i, 0, 0))
        weight_out = pl.BlockSpec((1, d_ff, d_model), lambda i, first=first: (first + i, 0, 0))
        row_block = pl.BlockSpec((capacity,) + row, lambda i: (i, 0, 0))
        tables = arrived[c] + [local[c]]
        n = len(tables)
        experts = pl.pallas_call(
            functools.partial(expert_kernel, n, len(grads), first, part, capacity, 512),
            grid=(part,),
            out_shape=[sds((part * capacity,) + row, BF16), sds(w_in.shape, BF16), sds(w_out.shape, BF16)],
            in_specs=[SMEM, SMEM, weight_in, weight_out] + [ANY] * (n + len(grads)),
            out_specs=[row_block, weight_in, weight_out],
            input_output_aliases={4 + n: 1, 5 + n: 2} if grads else {},
            scratch_shapes=[pltpu.VMEM((sum(t.shape[0] for t in tables),) + row, BF16), pltpu.VMEM((capacity,) + row, BF16), pltpu.VMEM((d_model // LANES, 2 * capacity, LANES), F32), pltpu.SemaphoreType.DMA((n,))],
            compiler_params=params(),
            cost_estimate=pl.CostEstimate(flops=12 * part * capacity * d_model * d_ff, bytes_accessed=8 * part * d_model * d_ff, transcendentals=part * capacity * d_ff),
            name='experts',
        )
        out_rows, *grads = experts(fill, recv, w_in, w_out, *tables, *grads)
        sib_out = to_sibling(out_rows)
        sent = pick([out_rows, sib_out], ret[c], [(m * half, half) for m in range(chips - 1)])
        got = [to_chip(v, m + 1) for m, v in enumerate(sent)]
        final += got + [to_sibling(v) for v in got] + [out_rows, sib_out]
    tile = 512
    wide = pl.BlockSpec((tile, d_model), lambda i: (i, 0))
    y_out, grad_x, grad_gate = pl.pallas_call(
        functools.partial(combine_kernel, tile, len(final)),
        grid=(n_tokens // tile,),
        out_shape=[sds(x_in.shape, BF16), sds(x_in.shape, BF16), sds((token_rows, LANES), F32)],
        in_specs=[SMEM, wide, VMEM, wide] + [ANY] * len(final),
        out_specs=[wide, wide, VMEM],
        scratch_shapes=[pltpu.VMEM((sum(t.shape[0] for t in final) + 8,) + row, BF16), pltpu.VMEM((tile,) + row, BF16), pltpu.VMEM((tile // LANES, d_model // LANES, 2 * LANES, LANES), F32), pltpu.SemaphoreType.DMA((len(final),))],
        compiler_params=params(), name='combine',
    )(fpos, x_in, gate, grad_y, *final)
    return y_out, grad_x, grad_gate.reshape(n_tokens, 1), grads[0], grads[1]


def solution(mesh):
    groups = mesh.shape['expert']
    tok_spec = P(('data', 'expert'), None)
    weight_spec = P('expert', None, None)
    grad_spec = P(('data', 'expert'), None, None)

    def device_pass(x_in, expert_idx, gate_weight, grad_y, w_in, w_out):
        sds = jax.ShapeDtypeStruct
        n_tokens, d_model = x_in.shape
        local_experts = w_in.shape[0]
        capacity = (CAP_NUM * n_tokens) // (CAP_DEN * local_experts)
        token_rows = n_tokens // LANES
        sibling = [(i, i ^ 1) for i in range(groups)]
        idx = expert_idx.reshape(token_rows, LANES)
        gate = gate_weight.reshape(token_rows, LANES)
        core = lax.rem(lax.axis_index('expert'), CORES)
        other = lax.ppermute(idx, 'expert', sibling)
        idx2 = jnp.where(core == 0, jnp.concatenate([idx, other]), jnp.concatenate([other, idx]))
        tile = 512
        wide = pl.BlockSpec((tile, d_model), lambda i: (i, 0))
        own_rows = pl.pallas_call(
            functools.partial(build_kernel, tile),
            grid=(n_tokens // tile,),
            out_shape=sds((n_tokens, 2, d_model), BF16),
            in_specs=[wide, VMEM, wide],
            out_specs=pl.BlockSpec((tile, 2, d_model), lambda i: (i, 0, 0)),
            scratch_shapes=[pltpu.VMEM((d_model // LANES, 2 * LANES, LANES), F32)] * (tile // LANES),
            compiler_params=params(), name='build',
        )(x_in, gate, grad_y)
        rank, every = pl.pallas_call(
            functools.partial(count_kernel, groups),
            out_shape=[sds((CORES * token_rows, LANES), I32), sds((groups, LANES), I32)],
            in_specs=[VMEM], out_specs=[VMEM] * 2,
            scratch_shapes=[pltpu.VMEM((8, LANES), I32), pltpu.VMEM((groups, 8, LANES), I32),
                            pltpu.SemaphoreType.DMA((groups,)), pltpu.SemaphoreType.DMA((groups,))],
            cost_estimate=pl.CostEstimate(flops=20 * 10 ** 6, bytes_accessed=10 ** 6, transcendentals=0),
            compiler_params=pltpu.CompilerParams(collective_id=0, has_side_effects=True), name='count',
        )(idx2)
        need = pl.pallas_call(
            functools.partial(need_kernel, capacity, local_experts),
            out_shape=sds((1, LANES), I32), in_specs=[VMEM], out_specs=VMEM, name='need',
        )(every)[0, 0]

        def by_lists(half):
            def run(x, g, i, *rest):
                return list_pass(groups, half, x, g, *rest)

            return run

        branches = [by_lists(half) for half in UNITS]
        branches.append(lambda x, g, i, dy, wi, wo, *rest: padded_pass(groups, x, i, g.reshape(n_tokens, 1), dy, wi, wo))
        which = sum((need > max(PARTS) * unit).astype(I32) for unit in UNITS)
        return lax.switch(which, branches, x_in, gate, expert_idx, grad_y, w_in, w_out, idx2, rank, every, own_rows)

    return jax.shard_map(device_pass, mesh=mesh,
                         in_specs=(tok_spec, tok_spec, tok_spec, tok_spec, weight_spec, weight_spec),
                         out_specs=(tok_spec, tok_spec, tok_spec, grad_spec, grad_spec), check_vma=False)
```
